512 devices in a mesh: ctx: 64 (over z, y), head: 8 (over x, core).
Axes of the slice: x: 4, y: 4, z: 16, core: 2. Of those that a mesh axis runs over, the one named last changes fastest.
Arguments:
- banded_queries: bfloat16 [16384, 4096], P('ctx', 'head'), may hold values from -11.5 to 11.5
- banded_keys: bfloat16 [16384, 512], P('ctx', 'head'), may hold values from -11.5 to 11.5
- banded_values: bfloat16 [16384, 512], P('ctx', 'head'), may hold values from -6 to 6
- full_queries: bfloat16 [16384, 4096], P('ctx', 'head'), may hold values from -11.5 to 11.5
- full_keys: bfloat16 [16384, 512], P('ctx', 'head'), may hold values from -11.5 to 11.5
- full_values: bfloat16 [16384, 512], P('ctx', 'head'), may hold values from -6 to 6
- segment_ids: int32 [16384], P('ctx'), may hold values from 0 to 16383, as said below
- position_ids: int32 [16384], P('ctx'), may hold values from 0 to 8189, as said below
- out_weight: bfloat16 [4096, 2880], P('head'), may hold values from -0.09375 to 0.09375
Outputs:
- banded_out: bfloat16 [16384, 4096], P('ctx', 'head')
- projected: bfloat16 [16384, 2880], P(('ctx', 'head'))
The draws below stay inside these ranges and needn't reach their ends.
Inputs may be any that keep to these rules, and one draw needn't show every extreme that they name: `segment_ids`: never falling; a document's id is the index of its last token; every document holds 1 to 3072 tokens, and one holds exactly 3072. `position_ids`: within a document they rise by 1 or 2 from one token to the next.
All inputs are finite; a program needn't handle non-finite values.
Results may differ from the reference program's by a relative error of at most 0.015.
The reference program's roundings to bfloat16 on the way count: a program that leaves them out, or rounds other values in their place, can miss the bound.
Values may be sent and summed in bfloat16 or wider, within the bound.
A program may use at most 64 MiB of HBM per device.

```python
import jax
import jax.numpy as jnp
from jax import lax

HEADS = 64
KV_HEADS = 8
HEAD_DIM = 64
D = 2880
WINDOW = 128
REACH = 12
TOK_DEV = 256
TOKENS = 16384
MOST = 3072
N_CTX = 64
N_HEAD = 8


def document_layout(key):
    key_first, key_kind, key_long, key_short, key_climb, key_offset = jax.random.split(key, 6)
    first_length = jax.random.randint(key_first, (), 1, min(MOST, TOKENS - MOST) + 1)
    kinds = jax.random.randint(key_kind, (TOKENS,), 0, 4)
    longer = jax.random.randint(key_long, (TOKENS,), max(MOST // 2, 1), MOST + 1)
    shorter = jax.random.randint(key_short, (TOKENS,), 1, max(MOST // 8, 1) + 1)
    lengths = jnp.where(kinds == 0, longer, shorter)
    lengths = lengths.at[0].set(first_length).at[1].set(MOST)
    doc_ends = jnp.cumsum(lengths)
    starts = doc_ends - lengths
    token_index = jnp.arange(TOKENS, dtype=jnp.int32)
    ordinal = jnp.searchsorted(doc_ends, token_index, side='right').astype(jnp.int32)
    segments = jnp.minimum(doc_ends[ordinal] - 1, TOKENS - 1).astype(jnp.int32)
    steps_drawn = jax.random.randint(key_climb, (TOKENS,), 1, 3)
    steps_drawn = jnp.where(ordinal == 1, 2, steps_drawn)
    climbs = jnp.cumsum(steps_drawn)
    offsets = jax.random.randint(key_offset, (TOKENS,), 0, 2048)
    offsets = offsets.at[1].set(2047)
    doc_first = starts[ordinal]
    positions = offsets[ordinal] + climbs - climbs[doc_first]
    return (segments, positions.astype(jnp.int32))


def drawn_pair(key):
    key_query, key_key = jax.random.split(key, 2)
    queries = jax.random.truncated_normal(key_query, -4.0, 4.0, (TOKENS, HEADS, HEAD_DIM), jnp.float32)
    key_rows = jax.random.truncated_normal(key_key, -4.0, 4.0, (TOKENS, KV_HEADS, HEAD_DIM), jnp.float32)
    return (queries.reshape(TOKENS, HEADS * HEAD_DIM), key_rows.reshape(TOKENS, KV_HEADS * HEAD_DIM))


def draw_banded_queries(key, part):
    return drawn_pair(jax.random.fold_in(key, 21))[0].astype(jnp.bfloat16)


def draw_banded_keys(key, part):
    return drawn_pair(jax.random.fold_in(key, 21))[1].astype(jnp.bfloat16)


def draw_full_queries(key, part):
    return drawn_pair(jax.random.fold_in(key, 22))[0].astype(jnp.bfloat16)


def draw_full_keys(key, part):
    return drawn_pair(jax.random.fold_in(key, 22))[1].astype(jnp.bfloat16)


def draw_segment_ids(key, part):
    return document_layout(jax.random.fold_in(key, 7))[0]


def draw_position_ids(key, part):
    return document_layout(jax.random.fold_in(key, 7))[1]


def block_scale(own_key, extent, cuts, least, top_value):
    def one(axis_at, shards_of):
        heights = jax.random.uniform(jax.random.fold_in(jax.random.fold_in(own_key, 6), axis_at), (shards_of,), jnp.float32, least / len(cuts), top_value / len(cuts))
        return jnp.repeat(jnp.exp(heights), extent[axis_at] // shards_of).reshape((-1,) + (1,) * (len(extent) - axis_at - 1))

    loudness = one(*cuts[0])
    for cut in cuts[1:]:
        loudness = loudness * one(*cut)
    return loudness


def bell_draw(key, shape, deviation, bound, pieces=(), kind=jnp.bfloat16):
    drawn = deviation * jax.random.normal(key, shape, jnp.float32)
    if pieces:
        drawn = drawn * block_scale(key, shape, pieces, -0.22, 0.18)
    return jnp.clip(drawn, -bound, bound).astype(kind)


def setup_inputs(seed: int = 0) -> dict:
    arg_keys = jax.random.split(jax.random.key(seed), 10)
    banded_queries = draw_banded_queries(jax.random.fold_in(arg_keys[9], 71), 0)
    banded_keys = draw_banded_keys(jax.random.fold_in(arg_keys[9], 71), 0)
    banded_values = bell_draw(arg_keys[2], (TOKENS, KV_HEADS * HEAD_DIM), 1.0, 6.0, ((0, 64), (1, 8)))
    full_queries = draw_full_queries(jax.random.fold_in(arg_keys[9], 71), 0)
    full_keys = draw_full_keys(jax.random.fold_in(arg_keys[9], 71), 0)
    full_values = bell_draw(arg_keys[5], (TOKENS, KV_HEADS * HEAD_DIM), 1.0, 6.0, ((0, 64), (1, 8)))
    segment_ids = draw_segment_ids(jax.random.fold_in(arg_keys[9], 71), 0)
    position_ids = draw_position_ids(jax.random.fold_in(arg_keys[9], 71), 0)
    out_weight = bell_draw(arg_keys[8], (HEADS * HEAD_DIM, D), (HEADS * HEAD_DIM) ** -0.5, 0.09375, ((0, 8),))
    return {"banded_queries": banded_queries, "banded_keys": banded_keys, "banded_values": banded_values, "full_queries": full_queries, "full_keys": full_keys, "full_values": full_values, "segment_ids": segment_ids, "position_ids": position_ids, "out_weight": out_weight}


theta_base = 150000.0
neg_fill = -1.0e30


def rotary(values_in, positions):
    row_count = values_in.shape[0]
    head_count = values_in.shape[1] // HEAD_DIM
    half_width = HEAD_DIM // 2
    frequency = theta_base ** (-2.0 * jnp.arange(half_width, dtype=jnp.float32) / HEAD_DIM)
    angles = positions.astype(jnp.float32)[:, None] * frequency[None, :]
    cosine = jnp.cos(angles)[:, None, :]
    sine_term = jnp.sin(angles)[:, None, :]
    spread = values_in.astype(jnp.float32).reshape(row_count, head_count, HEAD_DIM)
    leading = spread[..., :half_width]
    trailing = spread[..., half_width:]
    turned = jnp.concatenate([leading * cosine - trailing * sine_term, trailing * cosine + leading * sine_term], axis=-1)
    return turned.reshape(row_count, head_count * HEAD_DIM).astype(jnp.bfloat16)


def attend(queries, key_rows, value_rows, segment_ids, back_shards, window):
    group_size = HEADS // KV_HEADS
    pad_rows = back_shards * TOK_DEV
    span = (back_shards + 1) * TOK_DEV
    keys_padded = jnp.concatenate([jnp.zeros((pad_rows, key_rows.shape[1]), key_rows.dtype), key_rows], axis=0)
    values_padded = jnp.concatenate([jnp.zeros((pad_rows, value_rows.shape[1]), value_rows.dtype), value_rows], axis=0)
    segments_padded = jnp.concatenate([jnp.full((pad_rows,), -1, jnp.int32), segment_ids.astype(jnp.int32)])
    scale_factor = HEAD_DIM ** -0.5

    def one_shard(shard):
        row_start = (shard * TOK_DEV).astype(jnp.int32)
        query_block = lax.dynamic_slice_in_dim(queries, row_start, TOK_DEV, 0).astype(jnp.float32)
        query_block = query_block.reshape(TOK_DEV, KV_HEADS, group_size, HEAD_DIM)
        key_block = lax.dynamic_slice_in_dim(keys_padded, row_start, span, 0).astype(jnp.float32).reshape(span, KV_HEADS, HEAD_DIM)
        value_block = lax.dynamic_slice_in_dim(values_padded, row_start, span, 0).astype(jnp.float32).reshape(span, KV_HEADS, HEAD_DIM)
        query_segments = lax.dynamic_slice_in_dim(segment_ids.astype(jnp.int32), row_start, TOK_DEV, 0)
        key_segments = lax.dynamic_slice_in_dim(segments_padded, row_start, span, 0)
        query_index = row_start + jnp.arange(TOK_DEV, dtype=jnp.int32)
        key_index = row_start - pad_rows + jnp.arange(span, dtype=jnp.int32)
        allowed = (query_segments[:, None] == key_segments[None, :]) & (key_index[None, :] <= query_index[:, None])
        allowed = allowed & (key_index[None, :] >= 0) & (query_index[:, None] - key_index[None, :] < window)
        scores = jnp.einsum("qhgd,khd->hgqk", query_block, key_block) * scale_factor
        masked = jnp.where(allowed, scores, neg_fill)
        peak = jnp.max(masked, axis=-1, keepdims=True)
        weights = jnp.where(allowed, jnp.exp(masked - peak), 0.0)
        total = jnp.sum(weights, axis=-1, keepdims=True)
        rounded = lax.optimization_barrier(weights.astype(jnp.bfloat16)).astype(jnp.float32)
        mixed = jnp.einsum("hgqk,khd->hgqd", rounded, value_block) / total
        mixed = jnp.transpose(mixed, (2, 0, 1, 3)).reshape(TOK_DEV, HEADS * HEAD_DIM)
        return mixed.astype(jnp.bfloat16)

    blocks = lax.map(one_shard, jnp.arange(N_CTX, dtype=jnp.int32))
    return blocks.reshape(N_CTX * TOK_DEV, HEADS * HEAD_DIM)


def reference(banded_queries, banded_keys, banded_values, full_queries, full_keys, full_values, segment_ids, position_ids, out_weight):
    banded_q_rot = rotary(banded_queries, position_ids)
    banded_k_rot = rotary(banded_keys, position_ids)
    full_q_rot = rotary(full_queries, position_ids)
    full_k_rot = rotary(full_keys, position_ids)
    banded_out = attend(banded_q_rot, banded_k_rot, banded_values, segment_ids, 1, WINDOW)
    full_mixed = attend(full_q_rot, full_k_rot, full_values, segment_ids, REACH, MOST)
    group_width = HEADS * HEAD_DIM // N_HEAD
    summed = jnp.zeros((full_mixed.shape[0], D), jnp.float32)
    for group in range(N_HEAD):
        columns = full_mixed[:, group * group_width:(group + 1) * group_width]
        weight_rows = out_weight[group * group_width:(group + 1) * group_width]
        part_term = jnp.dot(columns, weight_rows, preferred_element_type=jnp.float32)
        summed = summed + lax.optimization_barrier(part_term.astype(jnp.bfloat16)).astype(jnp.float32)
    projected = summed.astype(jnp.bfloat16)
    return banded_out, projected
```

```python
import functools

import jax
import jax.numpy as jnp
import numpy as np
from jax import lax
from jax.experimental import pallas as pl
from jax.experimental.pallas import tpu as pltpu
from jax.sharding import PartitionSpec as P

f32 = jnp.float32
bf16 = jnp.bfloat16
MESH = pl.DeviceIdType.MESH

HEAD_DIM = 64
HALF = 32
WINDOW = 128
NY = 4
NX = 4
T = 256
G = 8
D = 2880
THETA = 150000.0
NEG = -1e30
Q_SCALE = float(np.log2(np.e) * HEAD_DIM**-0.5)
COLS = ((0, 768), (768, 768), (1536, 768), (2304, 576))
CHUNKS = ((0, 64), (64, 64))
NCH = len(CHUNKS)


def cos_sin(x):
    n = jnp.floor(x * f32(2.0 / np.pi) + 0.5)
    r = ((x - n * f32(1.5703125)) - n * f32(4.837512969970703125e-4)) - n * f32(7.549789954891882e-8)
    r2 = r * r
    s = r + r * r2 * (f32(-1.6666654611e-1) + r2 * (f32(8.3321608736e-3) + r2 * f32(-1.9515295891e-4)))
    c = (1.0 - 0.5 * r2) + r2 * r2 * (
        f32(4.166664568298827e-2) + r2 * (f32(-1.388731625493765e-3) + r2 * f32(2.443315711809948e-5))
    )
    k = n.astype(jnp.int32)
    odd = (k & 1) == 1
    sin_v = jnp.where(odd, c, s)
    cos_v = jnp.where(odd, s, c)
    sin_v = jnp.where((k & 2) == 2, -sin_v, sin_v)
    cos_v = jnp.where(((k + 1) & 2) == 2, -cos_v, cos_v)
    return cos_v, sin_v


def row_max(s3):
    n = s3.shape[0]
    parts = [jnp.max(s3[i * n // 4 : (i + 1) * n // 4], axis=0) for i in range(4)]
    mx = jnp.maximum(jnp.maximum(parts[0], parts[1]), jnp.maximum(parts[2], parts[3]))
    mx = jnp.maximum(mx, pltpu.roll(mx, 4, 0))
    mx = jnp.maximum(mx, pltpu.roll(mx, 2, 0))
    return jnp.maximum(mx, pltpu.roll(mx, 1, 0))


def kernel(
    n_ctx,
    bq_ref, bk_ref, bv_ref, fq_ref, fk_ref, fv_ref, seg_ref, pos_ref, freq_ref, w_hbm,
    band_out, proj_out,
    kvt, seg_all, kp, qf, qb, bkt, halo, halo_seg, bkp, bias_f, bias_b, m_s, acc, mixed, wv,
    part, rp, snd, rbuf, fin, keep,
    w_sem, z_send, y_send, kv_recv, halo_send, halo_recv, p_send, p_recv, x_send, x_recv,
):
    ctx = lax.axis_index("ctx")
    head = lax.axis_index("head")
    y = lax.rem(ctx, NY)
    core = lax.rem(head, 2)

    def wrap(i):
        return lax.rem(i + n_ctx, n_ctx)

    z_up, z_down = wrap(ctx + NY), wrap(ctx - NY)
    ys = [ctx - y + lax.rem(y + d, NY) for d in (1, 2, 3)]
    xs = [lax.rem(head + 2 * d, 2 * NX) for d in (1, 2, 3)]
    partner = head + 1 - 2 * core

    w_copy = pltpu.make_async_copy(w_hbm, wv, w_sem)
    w_copy.start()

    barrier = pltpu.get_barrier_semaphore()
    greet = [{"ctx": c} for c in (z_up, z_down, wrap(ctx + 1), wrap(ctx - 1), *ys)]
    greet += [{"head": h} for h in (*xs, partner)]
    for where in greet:
        pl.semaphore_signal(barrier, inc=1, device_id=where, device_id_type=MESH)

    pos = pos_ref[...].astype(f32)
    freq = freq_ref[...]
    cosine, sine = cos_sin(freq * pos)
    cos_q, sin_q = cosine * f32(Q_SCALE), sine * f32(Q_SCALE)

    def rotated(xt, c, s):
        a = xt[0:HALF].astype(f32)
        b = xt[HALF : 2 * HALF].astype(f32)
        return (a * c - b * s).astype(bf16), (b * c + a * s).astype(bf16)

    def store_kv(dst, k_ref, v_ref):
        kt = k_ref[...].T
        lo, hi = rotated(kt, cosine, sine)
        dst[0:HALF, :] = lo
        dst[HALF : 2 * HALF, :] = hi
        dst[64:128, :] = v_ref[...].T

    own = 3 * NY
    ones16 = jnp.ones((16, T), bf16)
    store_kv(kvt.at[own], fk_ref, fv_ref)
    store_kv(bkt, bk_ref, bv_ref)
    for s in range(own + 1):
        kvt[s, 128:144, :] = ones16
    bkt[128:144, :] = ones16
    seg_row = seg_ref[...]
    seg_all[own] = seg_row

    pl.semaphore_wait(barrier, len(greet))

    def kv_copies(src_slot, dst_slot, ssem, where):
        out = []
        for i, (lo, n) in enumerate(CHUNKS):
            out.append(pltpu.make_async_remote_copy(
                src_ref=kvt.at[src_slot, pl.ds(lo, n)], dst_ref=kvt.at[dst_slot, pl.ds(lo, n)],
                send_sem=ssem.at[i], recv_sem=kv_recv.at[dst_slot, i],
                device_id=where, device_id_type=MESH))
        out.append(pltpu.make_async_remote_copy(
            src_ref=seg_all.at[src_slot], dst_ref=seg_all.at[dst_slot],
            send_sem=ssem.at[NCH], recv_sem=kv_recv.at[dst_slot, NCH],
            device_id=where, device_id_type=MESH))
        return [out[-1]] + out[:-1]

    def z_copies(k):
        src = own if k == 0 else (k - 1) * NY + y
        return kv_copies(src, k * NY + y, z_send.at[k], {"ctx": z_up})

    def y_copies(k, d):
        src = own if k == 0 else (k - 1) * NY + y
        dst = 2 * NY + y if k == 0 else (k - 1) * NY + y
        return kv_copies(src, dst, y_send.at[k, d - 1], {"ctx": ys[d - 1]})

    def y_guard(k, d):
        if k == 0:
            return y + d < NY
        if k == 3:
            return y + d >= NY
        return None

    def y_start(k):
        for d in (1, 3, 2):
            g = y_guard(k, d)
            def go(d=d):
                for c in y_copies(k, d):
                    c.start()
            go() if g is None else pl.when(g)(go)

    def y_wait_send(k):
        for d in (1, 3, 2):
            g = y_guard(k, d)
            def go(d=d):
                for c in y_copies(k, d):
                    c.wait_send()
            go() if g is None else pl.when(g)(go)

    def wait_chunk(slot, i):
        if i < NCH:
            lo, n = CHUNKS[i]
            ref = kvt.at[slot, pl.ds(lo, n)]
        else:
            ref = seg_all.at[slot]
        pltpu.make_async_remote_copy(
            src_ref=ref, dst_ref=ref, send_sem=z_send.at[0, 0], recv_sem=kv_recv.at[slot, i],
            device_id={"ctx": z_up}, device_id_type=MESH).wait_recv()

    def wait_slot(slot):
        for i in (NCH, *range(NCH)):
            wait_chunk(slot, i)

    rim = pl.ds(T - WINDOW, WINDOW)
    halo_copies = [
        pltpu.make_async_remote_copy(
            src_ref=src, dst_ref=dst, send_sem=halo_send.at[i], recv_sem=halo_recv.at[i],
            device_id={"ctx": wrap(ctx + 1)}, device_id_type=MESH)
        for i, (src, dst) in enumerate((
            (bkt.at[pl.ds(0, 128), rim], halo), (seg_all.at[own, pl.ds(0, 1), rim], halo_seg)))
    ]

    for c in z_copies(0):
        c.start()
    y_start(0)
    for c in halo_copies:
        c.start()

    seg_f = seg_row.astype(f32)
    seg0 = seg_f[0:1, 0:1]
    row_bias = jnp.where(seg_f == seg0, f32(0), f32(NEG))
    i16 = lax.broadcasted_iota(jnp.int32, (16, T), 0)
    feat = jnp.where(i16 == 0, f32(1), jnp.where(i16 == 1, jnp.broadcast_to(row_bias, (16, T)), f32(0))).astype(bf16)
    zeros48 = jnp.zeros((48, 2048), bf16)
    qf[80:128, :] = zeros48
    qb[80:128, :] = zeros48
    qb[64:80, :] = jnp.zeros((16, 2048), bf16)

    def cols(h, g):
        return slice((h * G + g) * 128, (h * G + g + 1) * 128)

    def prep_q(dst, src):
        for j in range(G // 2):
            xt = src[:, j * 128 : (j + 1) * 128].T
            for e in range(2):
                lo, hi = rotated(xt[e * 64 : (e + 1) * 64], cos_q, sin_q)
                for h in range(2):
                    c = cols(h, 2 * j + e)
                    dst[0:HALF, c] = lo[:, h * 128 : (h + 1) * 128]
                    dst[HALF : 2 * HALF, c] = hi[:, h * 128 : (h + 1) * 128]

    prep_q(qf, fq_ref)
    for h in range(2):
        for g in range(G):
            qf[64:80, cols(h, g)] = feat[:, h * 128 : (h + 1) * 128]

    def key_rows(kt):
        n = kt.shape[1]
        return jnp.concatenate([kt, jnp.zeros((64, n), bf16)], axis=0).T

    def seg_cols(row128):
        return jnp.broadcast_to(row128, (128, 128)).T

    own_seg_cols = [seg_cols(seg_f[:, h * 128 : (h + 1) * 128]) for h in range(2)]
    ki = lax.broadcasted_iota(jnp.int32, (128, 128), 0)
    ti = lax.broadcasted_iota(jnp.int32, (128, 128), 1)
    for kh in range(2):
        for h in range(2):
            ok = (own_seg_cols[kh] == seg_f[:, h * 128 : (h + 1) * 128])
            if kh == h:
                ok = ok & (ki <= ti)
            if kh > h:
                ok = ok & (ki < 0)
            bias_f[kh * 128 : (kh + 1) * 128, h * 128 : (h + 1) * 128] = jnp.where(ok, f32(0), f32(NEG))

    kp[0:T, :] = key_rows(kvt[own, 0:64, :])

    def run_tiles(tiles, stage_a, stage_b, stage_c, lead=2):
        s, p = {}, {}
        for r in range(min(lead, len(tiles))):
            s[r] = stage_a(*tiles[r])
        for r in range(len(tiles)):
            if r + lead < len(tiles):
                s[r + lead] = stage_a(*tiles[r + lead])
            p[r] = stage_b(*tiles[r], s.pop(r))
            if r >= 1:
                stage_c(*tiles[r - 1], *p.pop(r - 1))
        stage_c(*tiles[-1], *p.pop(len(tiles) - 1))

    tiles = [(h, g) for h in range(2) for g in range(G)]

    def diag_a(h, g):
        return jnp.dot(kp[0:T, :], qf[:, cols(h, g)], preferred_element_type=f32) + bias_f[:, h * 128 : (h + 1) * 128]

    def diag_b(h, g, s):
        s3 = s.reshape(T // 8, 8, 128)
        mn = row_max(s3)
        m_s[:, cols(h, g)] = mn
        return (jnp.exp2(s3 - mn[None]).reshape(T, 128).astype(bf16),)

    def diag_c(h, g, p):
        acc[:, cols(h, g)] = jnp.dot(kvt[own, 64:144, :], p, preferred_element_type=f32)

    run_tiles(tiles, diag_a, diag_b, diag_c)

    wait_slot(0 * NY + y)
    for c in z_copies(1):
        c.start()
    y_start(1)

    prep_q(qb, bq_ref)
    for c in halo_copies:
        c.wait_recv()
    halo_seg_cols = seg_cols(halo_seg[...].astype(f32))
    same_h0 = [halo_seg_cols == seg_f[:, 0:128], own_seg_cols[0] == seg_f[:, 0:128]]
    same_h1 = [own_seg_cols[0] == seg_f[:, 128:256], own_seg_cols[1] == seg_f[:, 128:256]]
    for h, same in enumerate((same_h0, same_h1)):
        bias_b[0:128, h * 128 : (h + 1) * 128] = jnp.where(same[0] & (ki > ti), f32(0), f32(NEG))
        bias_b[128:256, h * 128 : (h + 1) * 128] = jnp.where(same[1] & (ki <= ti), f32(0), f32(NEG))
    bkp[0:128, :] = key_rows(halo[0:64, :])
    bkp[128:384, :] = key_rows(bkt[0:64, :])

    band_t = {}

    def band_a(h, g):
        return jnp.dot(bkp[h * 128 : h * 128 + 256, :], qb[:, cols(h, g)], preferred_element_type=f32) + bias_b[:, h * 128 : (h + 1) * 128]

    def band_b(h, g, s):
        s3 = s.reshape(T // 8, 8, 128)
        mn = row_max(s3)
        return (jnp.exp2(s3 - mn[None]).reshape(T, 128).astype(bf16),)

    def band_c(h, g, p):
        if h == 0:
            vt = jnp.concatenate([
                jnp.concatenate([halo[64:128, :], jnp.ones((16, 128), bf16)], axis=0), bkt[64:144, 0:128]], axis=1)
        else:
            vt = bkt[64:144, :]
        o = jnp.dot(vt, p, preferred_element_type=f32)
        band_t[h, g] = (o[0:64] * (1.0 / o[64:65])).astype(bf16)
        if g % 2 == 1:
            pair = jnp.concatenate([band_t.pop((h, g - 1)), band_t.pop((h, g))], axis=0)
            band_out[h * 128 : (h + 1) * 128, (g - 1) * 64 : (g + 1) * 64] = pair.T

    run_tiles(tiles, band_a, band_b, band_c)

    wait_slot(1 * NY + y)
    for c in z_copies(2):
        c.start()
    y_start(2)

    def group(k):
        base = (k - 1) * NY
        for i in range(NY):
            slot = base + i
            @pl.when(y != i)
            def _(slot=slot):
                wait_slot(slot)
            kb = jnp.where(seg_all[slot].astype(f32) == seg0, f32(0), f32(NEG))
            kfeat = jnp.where(i16 == 0, jnp.broadcast_to(kb, (16, T)), jnp.where(i16 == 1, f32(1), f32(0))).astype(bf16)
            full = jnp.concatenate([kvt[slot, 0:64, :], kfeat, jnp.zeros((48, T), bf16)], axis=0)
            kp[i * T : (i + 1) * T, :] = full.T

        def a(h, g):
            return jnp.dot(kp[...], qf[:, cols(h, g)], preferred_element_type=f32)

        def b(h, g, s):
            s3 = s.reshape(NY * T // 8, 8, 128)
            mo = m_s[:, cols(h, g)]
            mn = jnp.maximum(mo, row_max(s3))
            m_s[:, cols(h, g)] = mn
            return jnp.exp2(s3 - mn[None]).reshape(NY * T, 128).astype(bf16), jnp.exp2(mo - mn)

        def c(h, g, p, al):
            o = None
            for i in range(NY):
                t = jnp.dot(kvt[base + i, 64:144, :], p[i * T : (i + 1) * T], preferred_element_type=f32)
                o = t if o is None else o + t
            acc[:, cols(h, g)] = (acc[:, cols(h, g)].reshape(10, 8, 128) * al[None]).reshape(80, 128) + o

        run_tiles(tiles, a, b, c)

    group(1)
    wait_slot(2 * NY + y)
    y_start(3)
    group(2)
    group(3)

    for h in range(2):
        for g in range(0, G, 2):
            pair = []
            for e in range(2):
                o = acc[:, cols(h, g + e)]
                pair.append((o[0:64] * (1.0 / o[64:65])).astype(bf16))
            mixed[h * 128 : (h + 1) * 128, g * 64 : (g + 2) * 64] = jnp.concatenate(pair, axis=0).T

    w_copy.wait()

    def rows_of(c):
        return jnp.concatenate(
            [mixed[pl.ds(pl.multiple_of(64 * i + 32 * c, 32), 32), :] for i in range(NX)], axis=0)

    def p_copy(i):
        return pltpu.make_async_remote_copy(
            src_ref=part.at[0, pl.ds(32 * i, 32)], dst_ref=rp.at[pl.ds(32 * i, 32)],
            send_sem=p_send.at[i], recv_sem=p_recv.at[i], device_id={"head": partner}, device_id_type=MESH)

    for side, c in ((0, 1 - core), (1, core)):
        lhs = rows_of(c)
        for lo, n in COLS:
            part[side, :, lo : lo + n] = jnp.dot(lhs, wv[:, lo : lo + n], preferred_element_type=f32).astype(bf16)
        if side == 0:
            for i in range(NX):
                p_copy(i).start()
    for i in range(NX):
        p_copy(i).wait_recv()

    chip = head // 2
    far, up, down = [lax.rem(chip + d, NX) for d in (2, 1, 3)]

    def chip_sum(i):
        at = pl.ds(pl.multiple_of(32 * i, 32), 32)
        return part[1, at, :].astype(f32) + rp[at, :].astype(f32)

    def x_copy(n, src, dst, h):
        return pltpu.make_async_remote_copy(
            src_ref=src, dst_ref=dst, send_sem=x_send.at[n], recv_sem=x_recv.at[n],
            device_id={"head": h}, device_id_type=MESH)

    x_up, x_down = xs[0], xs[2]
    lo, hi = pl.ds(0, 16), pl.ds(16, 16)
    x_copies = [
        x_copy(0, snd.at[0, lo], rbuf.at[lo], x_up),
        x_copy(1, snd.at[0, hi], rbuf.at[hi], x_down),
        x_copy(2, snd.at[1, hi], fin.at[0, hi], x_up),
        x_copy(3, snd.at[2, lo], fin.at[1, lo], x_down),
        x_copy(4, snd.at[1, lo], fin.at[0, lo], x_up),
        x_copy(5, snd.at[2, hi], fin.at[1, hi], x_down),
    ]
    snd[0] = chip_sum(far).astype(bf16)
    x_copies[0].start()
    x_copies[1].start()
    s_up = chip_sum(up)
    snd[1, 16:32] = s_up[16:32].astype(bf16)
    x_copies[2].start()
    s_down = chip_sum(down)
    snd[2, 0:16] = s_down[0:16].astype(bf16)
    x_copies[3].start()
    keep[0:32] = chip_sum(chip)
    keep[32:48] = s_up[0:16]
    keep[48:64] = s_down[16:32]
    x_copies[0].wait_recv()
    snd[1, 0:16] = (keep[32:48] + rbuf[0:16].astype(f32)).astype(bf16)
    x_copies[4].start()
    x_copies[1].wait_recv()
    snd[2, 16:32] = (keep[48:64] + rbuf[16:32].astype(f32)).astype(bf16)
    x_copies[5].start()
    for n in (2, 3, 4, 5):
        x_copies[n].wait_recv()
    proj_out[...] = (keep[0:32] + (fin[0].astype(f32) + fin[1].astype(f32))).astype(bf16)

    for k in range(3):
        for c in z_copies(k):
            c.wait_send()
    for k in range(4):
        y_wait_send(k)
    for c in halo_copies:
        c.wait_send()
    for i in range(NX):
        p_copy(i).wait_send()
    for c in x_copies:
        c.wait_send()


def body(n_ctx, bq, bk, bv, fq, fk, fv, seg, pos, w):
    freq = THETA ** (-2.0 * np.arange(HALF, dtype=np.float64) / HEAD_DIM)
    freq = jnp.asarray(np.broadcast_to(freq.astype(np.float32)[:, None], (HALF, T)))
    vmem = pl.BlockSpec(memory_space=pltpu.VMEM)
    dma = pltpu.SemaphoreType.DMA
    return pl.pallas_call(
        functools.partial(kernel, n_ctx),
        out_shape=(jax.ShapeDtypeStruct((T, G * HEAD_DIM), bf16), jax.ShapeDtypeStruct((32, D), bf16)),
        in_specs=[vmem] * 9 + [pl.BlockSpec(memory_space=pl.ANY)],
        out_specs=(vmem, vmem),
        scratch_shapes=[
            pltpu.VMEM((13, 144, T), bf16),
            pltpu.VMEM((13, 1, T), jnp.int32),
            pltpu.VMEM((NY * T, 128), bf16),
            pltpu.VMEM((128, 2048), bf16),
            pltpu.VMEM((128, 2048), bf16),
            pltpu.VMEM((144, T), bf16),
            pltpu.VMEM((128, 128), bf16),
            pltpu.VMEM((1, 128), jnp.int32),
            pltpu.VMEM((384, 128), bf16),
            pltpu.VMEM((T, T), f32),
            pltpu.VMEM((T, T), f32),
            pltpu.VMEM((8, 2048), f32),
            pltpu.VMEM((80, 2048), f32),
            pltpu.VMEM((T, 512), bf16),
            pltpu.VMEM((512, D), bf16),
            pltpu.VMEM((2, 128, D), bf16),
            pltpu.VMEM((128, D), bf16),
            pltpu.VMEM((3, 32, D), bf16),
            pltpu.VMEM((32, D), bf16),
            pltpu.VMEM((2, 32, D), bf16),
            pltpu.VMEM((64, D), f32),
            dma,
            dma((3, NCH + 1)),
            dma((4, 3, NCH + 1)),
            dma((12, NCH + 1)),
            dma((2,)),
            dma((2,)),
            dma((NX,)),
            dma((NX,)),
            dma((6,)),
            dma((6,)),
        ],
        compiler_params=pltpu.CompilerParams(
            collective_id=0, has_side_effects=True, vmem_limit_bytes=60000 * 1024),
        name="packed_attention",
    )(bq, bk, bv, fq, fk, fv, seg.reshape(1, T), pos.reshape(1, T), freq, w)


def solution(mesh):
    return jax.shard_map(
        functools.partial(body, mesh.shape["ctx"]),
        mesh=mesh,
        in_specs=(
            P("ctx", "head"),
            P("ctx", "head"),
            P("ctx", "head"),
            P("ctx", "head"),
            P("ctx", "head"),
            P("ctx", "head"),
            P("ctx"),
            P("ctx"),
            P("head", None),
        ),
        out_specs=(P("ctx", "head"), P(("ctx", "head"), None)),
        check_vma=False,
    )
```

```python
import functools

import jax
import jax.numpy as jnp
import numpy as np
from jax import lax
from jax.experimental import pallas as pl
from jax.experimental.pallas import tpu as pltpu
from jax.sharding import PartitionSpec as P

f32 = jnp.float32
bf16 = jnp.bfloat16
MESH = pl.DeviceIdType.MESH

HEAD_DIM = 64
HALF = 32
WINDOW = 128
NY = 4
NX = 4
T = 256
G = 8
D = 2880
THETA = 150000.0
NEG = -1e30
Q_SCALE = float(np.log2(np.e) * HEAD_DIM**-0.5)
COLS = ((0, 768), (768, 768), (1536, 768), (2304, 576))


def cos_sin(x):
    n = jnp.floor(x * f32(2.0 / np.pi) + 0.5)
    r = ((x - n * f32(1.5703125)) - n * f32(4.837512969970703125e-4)) - n * f32(7.549789954891882e-8)
    r2 = r * r
    s = r + r * r2 * (f32(-1.6666654611e-1) + r2 * (f32(8.3321608736e-3) + r2 * f32(-1.9515295891e-4)))
    c = (1.0 - 0.5 * r2) + r2 * r2 * (
        f32(4.166664568298827e-2) + r2 * (f32(-1.388731625493765e-3) + r2 * f32(2.443315711809948e-5))
    )
    k = n.astype(jnp.int32)
    odd = (k & 1) == 1
    sin_v = jnp.where(odd, c, s)
    cos_v = jnp.where(odd, s, c)
    sin_v = jnp.where((k & 2) == 2, -sin_v, sin_v)
    cos_v = jnp.where(((k + 1) & 2) == 2, -cos_v, cos_v)
    return cos_v, sin_v


def row_max(s3):
    n = s3.shape[0]
    parts = [jnp.max(s3[i * n // 4 : (i + 1) * n // 4], axis=0) for i in range(4)]
    mx = jnp.maximum(jnp.maximum(parts[0], parts[1]), jnp.maximum(parts[2], parts[3]))
    mx = jnp.maximum(mx, pltpu.roll(mx, 4, 0))
    mx = jnp.maximum(mx, pltpu.roll(mx, 2, 0))
    return jnp.maximum(mx, pltpu.roll(mx, 1, 0))


def kernel(
    n_ctx,
    bq_hbm, bk_hbm, bv_hbm, fq_hbm, fk_hbm, fv_hbm, seg_hbm, pos_hbm, w_hbm,
    band_out, proj_out,
    bq_ref, bk_ref, bv_ref, fq_ref, fk_ref, fv_ref, seg_ref, pos_ref,
    kvt, seg_all, kp, qf, qb, bkt, halo, halo_seg, bkp, bias_f, bias_b, m_s, acc, mixed, wv, wt,
    part, rp, snd, rbuf, fin, keep,
    in_sem, z_send, y_send, kv_recv, halo_send, halo_recv, p_send, p_recv, x_send, x_recv,
):
    ctx = lax.axis_index("ctx")
    head = lax.axis_index("head")
    y = lax.rem(ctx, NY)
    z = ctx // NY
    n_z = n_ctx // NY
    core = lax.rem(head, 2)

    ys = [ctx - y + lax.rem(y + d, NY) for d in (1, 2, 3)]
    xs = [lax.rem(head + 2 * d, 2 * NX) for d in (1, 2, 3)]
    partner = head + 1 - 2 * core

    loads = [
        pltpu.make_async_copy(src, dst, in_sem.at[i])
        for i, (src, dst) in enumerate((
            (fk_hbm, fk_ref), (pos_hbm, pos_ref), (fv_hbm, fv_ref), (seg_hbm, seg_ref), (bk_hbm, bk_ref),
            (bv_hbm, bv_ref), (fq_hbm, fq_ref), (bq_hbm, bq_ref), (w_hbm, wv)))
    ]
    for c in loads:
        c.start()

    def greet(where):
        pl.semaphore_signal(pltpu.get_barrier_semaphore(), inc=1, device_id=where, device_id_type=MESH)

    for c in ys:
        greet({"ctx": c})
    for h in (*xs, partner):
        greet({"head": h})
    met = jnp.int32(7)
    for there, c in ((z > 0, ctx - NY), (z < n_z - 1, ctx + NY), (ctx > 0, ctx - 1), (ctx < n_ctx - 1, ctx + 1)):
        pl.when(there)(lambda c=c: greet({"ctx": c}))
        met = met + there.astype(jnp.int32)

    own = 3 * NY

    def present(k, d):
        if k < 3:
            return z >= k
        return z >= 3 if d == 0 else (y >= d) | (z >= 3)

    for k in (1, 2, 3):
        for d in range(NY):
            @pl.when(jnp.logical_not(present(k, d)))
            def _(slot=4 * (k - 1) + d):
                kvt[slot, 0:128, :] = jnp.zeros((128, T), bf16)
                seg_all[slot] = jnp.full((1, T), -1, jnp.int32)

    @pl.when(ctx == 0)
    def _():
        halo[...] = jnp.zeros((128, 128), bf16)
        halo_seg[...] = jnp.full((1, 128), -1, jnp.int32)

    ones16 = jnp.ones((16, T), bf16)
    for i in range(own + 1):
        kvt[i, 128:144, :] = ones16
    bkt[128:144, :] = ones16
    fi = lax.broadcasted_iota(jnp.int32, (HALF, T), 0)
    freq = jnp.ones((HALF, T), f32)
    for i in range(1, HALF):
        freq = jnp.where(fi == i, f32(np.float32(THETA ** (-2.0 * i / HEAD_DIM))), freq)

    loads[0].wait()
    loads[1].wait()
    pos = pos_ref[...].astype(f32)
    cosine, sine = cos_sin(freq * pos)
    cos_q, sin_q = cosine * f32(Q_SCALE), sine * f32(Q_SCALE)

    def rotated(xt, c, s):
        a = xt[0:HALF].astype(f32)
        b = xt[HALF : 2 * HALF].astype(f32)
        return (a * c - b * s).astype(bf16), (b * c + a * s).astype(bf16)

    def store_kv(dst, k_ref, v_ref):
        lo, hi = rotated(k_ref[...], cosine, sine)
        dst[0:HALF, :] = lo
        dst[HALF : 2 * HALF, :] = hi
        dst[64:128, :] = v_ref[...]

    for c in loads[2:6]:
        c.wait()
    store_kv(kvt.at[own], fk_ref, fv_ref)
    store_kv(bkt, bk_ref, bv_ref)
    seg_row = seg_ref[...]
    seg_all[own] = seg_row

    pl.semaphore_wait(pltpu.get_barrier_semaphore(), met)

    K_ROWS, V_ROWS, SEG = 0, 1, 2

    def piece(slot, i):
        return seg_all.at[slot] if i == SEG else kvt.at[slot, pl.ds(64 * i, 64)]

    def send(src_slot, dst_slot, i, ssem, where):
        return pltpu.make_async_remote_copy(
            src_ref=piece(src_slot, i), dst_ref=piece(dst_slot, i), send_sem=ssem, recv_sem=kv_recv.at[dst_slot, i],
            device_id={"ctx": where}, device_id_type=MESH)

    def slot_of(k, d):
        return own if k == 0 else 4 * (k - 1) + d

    def z_copy(k, i):
        return send(slot_of(k, 0), slot_of(k + 1, 0), i, z_send.at[k, i], ctx + NY)

    def z_guard(k):
        return (z >= k) & (z < n_z - 1)

    def z_start(k, i):
        pl.when(z_guard(k))(lambda: z_copy(k, i).start())

    def y_copy(k, d, i):
        if k in (1, 2) and d == 2:
            via, to = (3, 2) if i == V_ROWS else (1, 0)
            return send(slot_of(k, via), slot_of(k, 2), i, y_send.at[k, 1, i], ys[to])
        return send(slot_of(k, 0), slot_of(k or 3, d), i, y_send.at[k, d - 1, i], ys[d - 1])

    def y_guard(k, d):
        if k == 0:
            return y + d < NY
        if k == 3:
            return (y + d >= NY) & (z >= 3)
        return z >= k

    def y_start(k, d, i):
        pl.when(y_guard(k, d))(lambda: y_copy(k, d, i).start())

    def recv(slot, i):
        ref = piece(slot, i)
        pltpu.make_async_remote_copy(
            src_ref=ref, dst_ref=ref, send_sem=z_send.at[0, 0], recv_sem=kv_recv.at[slot, i],
            device_id={"head": partner}, device_id_type=MESH).wait_recv()

    def arrive(k, d, i):
        pl.when(present(k, d))(lambda: recv(slot_of(k, d), i))

    rim = pl.ds(T - WINDOW, WINDOW)
    halo_copies = [
        pltpu.make_async_remote_copy(
            src_ref=src, dst_ref=dst, send_sem=halo_send.at[i], recv_sem=halo_recv.at[i],
            device_id={"ctx": ctx + 1}, device_id_type=MESH)
        for i, (src, dst) in enumerate((
            (bkt.at[pl.ds(0, 128), rim], halo), (seg_all.at[own, pl.ds(0, 1), rim], halo_seg)))
    ]

    for i in (SEG, K_ROWS, V_ROWS):
        z_start(0, i)

    @pl.when(ctx < n_ctx - 1)
    def _():
        for c in halo_copies:
            c.start()

    for d in (1, 3, 2):
        for i in (SEG, K_ROWS, V_ROWS):
            y_start(0, d, i)

    def relay(k):
        arrive(k, 0, SEG)
        arrive(k, 0, K_ROWS)
        if k < 3:
            z_start(k, SEG)
            z_start(k, K_ROWS)
        y_start(k, 1, SEG)
        y_start(k, 3, SEG)
        y_start(k, 1, K_ROWS)
        arrive(k, 0, V_ROWS)
        if k < 3:
            z_start(k, V_ROWS)
        y_start(k, 3, V_ROWS)
        y_start(k, 1, V_ROWS)
        y_start(k, 3, K_ROWS)
        if k == 3:
            for i in (SEG, K_ROWS, V_ROWS):
                y_start(3, 2, i)

    def across(k):
        arrive(k, 1, SEG)
        arrive(k, 1, K_ROWS)
        y_start(k, 2, SEG)
        y_start(k, 2, K_ROWS)
        arrive(k, 3, V_ROWS)
        y_start(k, 2, V_ROWS)

    seg_f = seg_row.astype(f32)
    seg0 = seg_f[0:1, 0:1]
    row_bias = jnp.where(seg_f == seg0, f32(0), f32(NEG))
    i16 = lax.broadcasted_iota(jnp.int32, (16, T), 0)
    feat = jnp.where(i16 == 0, f32(1), jnp.where(i16 == 1, jnp.broadcast_to(row_bias, (16, T)), f32(0))).astype(bf16)
    zeros48 = jnp.zeros((48, 2048), bf16)
    qf[80:128, :] = zeros48
    qb[80:128, :] = zeros48
    qb[64:80, :] = jnp.zeros((16, 2048), bf16)

    def cols(h, g):
        return slice((h * G + g) * 128, (h * G + g + 1) * 128)

    def prep_q(dst, src):
        for j in range(G // 2):
            xt = src[:, j * 128 : (j + 1) * 128].T
            for e in range(2):
                lo, hi = rotated(xt[e * 64 : (e + 1) * 64], cos_q, sin_q)
                for h in range(2):
                    c = cols(h, 2 * j + e)
                    dst[0:HALF, c] = lo[:, h * 128 : (h + 1) * 128]
                    dst[HALF : 2 * HALF, c] = hi[:, h * 128 : (h + 1) * 128]

    loads[6].wait()
    prep_q(qf, fq_ref)
    for h in range(2):
        for g in range(G):
            qf[64:80, cols(h, g)] = feat[:, h * 128 : (h + 1) * 128]

    def key_rows(kt):
        n = kt.shape[1]
        return jnp.concatenate([kt, jnp.zeros((64, n), bf16)], axis=0).T

    def seg_cols(row128):
        return jnp.broadcast_to(row128, (128, 128)).T

    own_seg_cols = [seg_cols(seg_f[:, h * 128 : (h + 1) * 128]) for h in range(2)]
    ki = lax.broadcasted_iota(jnp.int32, (128, 128), 0)
    ti = lax.broadcasted_iota(jnp.int32, (128, 128), 1)
    for kh in range(2):
        for h in range(2):
            ok = (own_seg_cols[kh] == seg_f[:, h * 128 : (h + 1) * 128])
            if kh == h:
                ok = ok & (ki <= ti)
            if kh > h:
                ok = ok & (ki < 0)
            bias_f[kh * 128 : (kh + 1) * 128, h * 128 : (h + 1) * 128] = jnp.where(ok, f32(0), f32(NEG))

    kp[0:T, :] = key_rows(kvt[own, 0:64, :])

    def run_tiles(tiles, stage_a, stage_b, stage_c, lead=3):
        s, p = {}, {}
        for r in range(min(lead, len(tiles))):
            s[r] = stage_a(*tiles[r])
        for r in range(len(tiles)):
            if r + lead < len(tiles):
                s[r + lead] = stage_a(*tiles[r + lead])
            p[r] = stage_b(*tiles[r], s.pop(r))
            if r >= 1:
                stage_c(*tiles[r - 1], *p.pop(r - 1))
        stage_c(*tiles[-1], *p.pop(len(tiles) - 1))

    tiles = [(h, g) for h in range(2) for g in range(G)]

    def diag_a(h, g):
        return jnp.dot(kp[0:T, :], qf[:, cols(h, g)], preferred_element_type=f32) + bias_f[:, h * 128 : (h + 1) * 128]

    def diag_b(h, g, s):
        s3 = s.reshape(T // 8, 8, 128)
        mn = row_max(s3)
        m_s[:, cols(h, g)] = mn
        return (jnp.exp2(s3 - mn[None]).reshape(T, 128).astype(bf16),)

    def diag_c(h, g, p):
        acc[:, cols(h, g)] = jnp.dot(kvt[own, 64:144, :], p, preferred_element_type=f32)

    run_tiles(tiles, diag_a, diag_b, diag_c)

    loads[8].wait()
    for j in range(0, D, 128):
        n = min(128, D - j)
        wt[:, j : j + n] = wv[j : j + n, :].T

    relay(1)

    loads[7].wait()
    prep_q(qb, bq_ref)

    @pl.when(ctx > 0)
    def _():
        for c in halo_copies:
            c.wait_recv()

    halo_seg_cols = seg_cols(halo_seg[...].astype(f32))
    same_h0 = [halo_seg_cols == seg_f[:, 0:128], own_seg_cols[0] == seg_f[:, 0:128]]
    same_h1 = [own_seg_cols[0] == seg_f[:, 128:256], own_seg_cols[1] == seg_f[:, 128:256]]
    for h, same in enumerate((same_h0, same_h1)):
        bias_b[0:128, h * 128 : (h + 1) * 128] = jnp.where(same[0] & (ki > ti), f32(0), f32(NEG))
        bias_b[128:256, h * 128 : (h + 1) * 128] = jnp.where(same[1] & (ki <= ti), f32(0), f32(NEG))
    bkp[0:128, :] = key_rows(halo[0:64, :])
    bkp[128:384, :] = key_rows(bkt[0:64, :])

    band_t = {}

    def band_a(h, g):
        return jnp.dot(bkp[h * 128 : h * 128 + 256, :], qb[:, cols(h, g)], preferred_element_type=f32) + bias_b[:, h * 128 : (h + 1) * 128]

    def band_b(h, g, s):
        s3 = s.reshape(T // 8, 8, 128)
        mn = row_max(s3)
        return (jnp.exp2(s3 - mn[None]).reshape(T, 128).astype(bf16),)

    def band_c(h, g, p):
        if h == 0:
            vt = jnp.concatenate([
                jnp.concatenate([halo[64:128, :], jnp.ones((16, 128), bf16)], axis=0), bkt[64:144, 0:128]], axis=1)
        else:
            vt = bkt[64:144, :]
        o = jnp.dot(vt, p, preferred_element_type=f32)
        band_t[h, g] = (o[0:64] * (1.0 / o[64:65])).astype(bf16)
        if g % 2 == 1:
            pair = jnp.concatenate([band_t.pop((h, g - 1)), band_t.pop((h, g))], axis=0)
            band_out[h * 128 : (h + 1) * 128, (g - 1) * 64 : (g + 1) * 64] = pair.T

    run_tiles(tiles, band_a, band_b, band_c)

    def group(members):
        for n, (k, d, pieces) in enumerate(members):
            slot = slot_of(k, d)
            for i in pieces:
                arrive(k, d, i)
            kb = jnp.where(seg_all[slot].astype(f32) == seg0, f32(0), f32(NEG))
            kfeat = jnp.where(i16 == 0, jnp.broadcast_to(kb, (16, T)), jnp.where(i16 == 1, f32(1), f32(0))).astype(bf16)
            full = jnp.concatenate([kvt[slot, 0:64, :], kfeat, jnp.zeros((48, T), bf16)], axis=0)
            kp[n * T : (n + 1) * T, :] = full.T

        def a(h, g):
            return jnp.dot(kp[...], qf[:, cols(h, g)], preferred_element_type=f32)

        def b(h, g, s):
            s3 = s.reshape(NY * T // 8, 8, 128)
            mo = m_s[:, cols(h, g)]
            mn = jnp.maximum(mo, row_max(s3))
            m_s[:, cols(h, g)] = mn
            return jnp.exp2(s3 - mn[None]).reshape(NY * T, 128).astype(bf16), jnp.exp2(mo - mn)

        def c(h, g, p, al):
            o = None
            for n, (k, d, _) in enumerate(members):
                t = jnp.dot(kvt[slot_of(k, d), 64:144, :], p[n * T : (n + 1) * T], preferred_element_type=f32)
                o = t if o is None else o + t
            acc[:, cols(h, g)] = (acc[:, cols(h, g)].reshape(10, 8, 128) * al[None]).reshape(80, 128) + o

        run_tiles(tiles, a, b, c)

    every = (SEG, K_ROWS, V_ROWS)
    relay(2)
    across(1)
    group(((1, 0, ()), (1, 1, (V_ROWS,)), (1, 3, (SEG, K_ROWS)), (2, 0, ())))
    relay(3)
    across(2)
    group(((1, 2, every), (2, 1, (V_ROWS,)), (2, 3, (SEG, K_ROWS)), (3, 0, ())))
    group(((2, 2, every), (3, 1, every), (3, 3, every), (3, 2, every)))

    for h in range(2):
        for g in range(0, G, 2):
            pair = []
            for e in range(2):
                o = acc[:, cols(h, g + e)]
                pair.append((o[0:64] * (1.0 / o[64:65])).astype(bf16))
            mixed[h * 128 : (h + 1) * 128, g * 64 : (g + 2) * 64] = jnp.concatenate(pair, axis=0).T


    def rows_of(c):
        return jnp.concatenate(
            [mixed[pl.ds(pl.multiple_of(64 * i + 32 * c, 32), 32), :] for i in range(NX)], axis=0)

    def p_copy(i):
        lo, n = COLS[i]
        return pltpu.make_async_remote_copy(
            src_ref=part.at[pl.ds(0, 128), pl.ds(lo, n)], dst_ref=rp.at[pl.ds(0, 128), pl.ds(lo, n)],
            send_sem=p_send.at[i], recv_sem=p_recv.at[i], device_id={"head": partner}, device_id_type=MESH)

    lhs = jnp.concatenate([rows_of(1 - core), rows_of(core)], axis=0)
    for i, (lo, n) in enumerate(COLS):
        part[:, lo : lo + n] = jnp.dot(lhs, wt[:, lo : lo + n], preferred_element_type=f32).astype(bf16)
        p_copy(i).start()
    for i in range(len(COLS)):
        p_copy(i).wait_recv()

    chip = head // 2
    far, up, down = [lax.rem(chip + d, NX) for d in (2, 1, 3)]

    def chip_sum(i):
        at = pl.ds(pl.multiple_of(32 * i, 32), 32)
        own_at = pl.ds(pl.multiple_of(128 + 32 * i, 32), 32)
        return part[own_at, :].astype(f32) + rp[at, :].astype(f32)

    def x_copy(n, src, dst, h):
        return pltpu.make_async_remote_copy(
            src_ref=src, dst_ref=dst, send_sem=x_send.at[n], recv_sem=x_recv.at[n],
            device_id={"head": h}, device_id_type=MESH)

    x_up, x_down = xs[0], xs[2]
    lo, hi = pl.ds(0, 16), pl.ds(16, 16)
    x_copies = [
        x_copy(0, snd.at[0, lo], rbuf.at[lo], x_up),
        x_copy(1, snd.at[0, hi], rbuf.at[hi], x_down),
        x_copy(2, snd.at[1, hi], fin.at[0, hi], x_up),
        x_copy(3, snd.at[2, lo], fin.at[1, lo], x_down),
        x_copy(4, snd.at[1, lo], fin.at[0, lo], x_up),
        x_copy(5, snd.at[2, hi], fin.at[1, hi], x_down),
    ]
    snd[0] = chip_sum(far).astype(bf16)
    x_copies[0].start()
    x_copies[1].start()
    s_up = chip_sum(up)
    snd[1, 16:32] = s_up[16:32].astype(bf16)
    x_copies[2].start()
    s_down = chip_sum(down)
    snd[2, 0:16] = s_down[0:16].astype(bf16)
    x_copies[3].start()
    keep[0:32] = chip_sum(chip)
    keep[32:48] = s_up[0:16]
    keep[48:64] = s_down[16:32]
    x_copies[0].wait_recv()
    snd[1, 0:16] = (keep[32:48] + rbuf[0:16].astype(f32)).astype(bf16)
    x_copies[4].start()
    x_copies[1].wait_recv()
    snd[2, 16:32] = (keep[48:64] + rbuf[16:32].astype(f32)).astype(bf16)
    x_copies[5].start()
    for n in (2, 3, 4, 5):
        x_copies[n].wait_recv()
    proj_out[...] = (keep[0:32] + (fin[0].astype(f32) + fin[1].astype(f32))).astype(bf16)

    for i in (SEG, K_ROWS, V_ROWS):
        for k in range(3):
            pl.when(z_guard(k))(lambda: z_copy(k, i).wait_send())
        for k in range(4):
            for d in (1, 2, 3):
                pl.when(y_guard(k, d))(lambda: y_copy(k, d, i).wait_send())

    @pl.when(ctx < n_ctx - 1)
    def _():
        for c in halo_copies:
            c.wait_send()

    for i in range(len(COLS)):
        p_copy(i).wait_send()
    for c in x_copies:
        c.wait_send()


def body(n_ctx, bq, bk, bv, fq, fk, fv, seg, pos, w):
    vmem = pl.BlockSpec(memory_space=pltpu.VMEM)
    dma = pltpu.SemaphoreType.DMA
    return pl.pallas_call(
        functools.partial(kernel, n_ctx),
        out_shape=(jax.ShapeDtypeStruct((T, G * HEAD_DIM), bf16), jax.ShapeDtypeStruct((32, D), bf16)),
        in_specs=[pl.BlockSpec(memory_space=pl.ANY)] * 9,
        out_specs=(vmem, vmem),
        scratch_shapes=[
            pltpu.VMEM((T, 512), bf16),
            pltpu.VMEM((64, T), bf16),
            pltpu.VMEM((64, T), bf16),
            pltpu.VMEM((T, 512), bf16),
            pltpu.VMEM((64, T), bf16),
            pltpu.VMEM((64, T), bf16),
            pltpu.VMEM((1, T), jnp.int32),
            pltpu.VMEM((1, T), jnp.int32),
            pltpu.VMEM((13, 144, T), bf16),
            pltpu.VMEM((13, 1, T), jnp.int32),
            pltpu.VMEM((NY * T, 128), bf16),
            pltpu.VMEM((128, 2048), bf16),
            pltpu.VMEM((128, 2048), bf16),
            pltpu.VMEM((144, T), bf16),
            pltpu.VMEM((128, 128), bf16),
            pltpu.VMEM((1, 128), jnp.int32),
            pltpu.VMEM((384, 128), bf16),
            pltpu.VMEM((T, T), f32),
            pltpu.VMEM((T, T), f32),
            pltpu.VMEM((8, 2048), f32),
            pltpu.VMEM((80, 2048), f32),
            pltpu.VMEM((T, 512), bf16),
            pltpu.VMEM((D, 512), bf16),
            pltpu.VMEM((512, D), bf16),
            pltpu.VMEM((2 * 128, D), bf16),
            pltpu.VMEM((128, D), bf16),
            pltpu.VMEM((3, 32, D), bf16),
            pltpu.VMEM((32, D), bf16),
            pltpu.VMEM((2, 32, D), bf16),
            pltpu.VMEM((64, D), f32),
            dma((9,)),
            dma((3, 3)),
            dma((4, 3, 3)),
            dma((12, 3)),
            dma((2,)),
            dma((2,)),
            dma((len(COLS),)),
            dma((len(COLS),)),
            dma((6,)),
            dma((6,)),
        ],
        compiler_params=pltpu.CompilerParams(
            collective_id=0, has_side_effects=True, vmem_limit_bytes=60000 * 1024),
        name="packed_attention",
    )(bq, bk.T, bv.T, fq, fk.T, fv.T, seg.reshape(1, T), pos.reshape(1, T), w.T)


def solution(mesh):
    return jax.shard_map(
        functools.partial(body, mesh.shape["ctx"]),
        mesh=mesh,
        in_specs=(
            P("ctx", "head"),
            P("ctx", "head"),
            P("ctx", "head"),
            P("ctx", "head"),
            P("ctx", "head"),
            P("ctx", "head"),
            P("ctx"),
            P("ctx"),
            P("head", None),
        ),
        out_specs=(P("ctx", "head"), P(("ctx", "head"), None)),
        check_vma=False,
    )
```

```python
import functools

import jax
import jax.numpy as jnp
import numpy as np
from jax import lax
from jax.experimental import pallas as pl
from jax.experimental.pallas import tpu as pltpu
from jax.sharding import PartitionSpec as P

f32 = jnp.float32
bf16 = jnp.bfloat16
MESH = pl.DeviceIdType.MESH

HEAD_DIM = 64
HALF = 32
WINDOW = 128
NY = 4
NX = 4
T = 256
G = 8
D = 2880
THETA = 150000.0
NEG = -1e30
Q_SCALE = float(np.log2(np.e) * HEAD_DIM**-0.5)
SPLIT = 1408
COLS = ((0, 1536), (1536, 1344))


def cos_sin(x):
    n = jnp.floor(x * f32(2.0 / np.pi) + 0.5)
    r = ((x - n * f32(1.5703125)) - n * f32(4.837512969970703125e-4)) - n * f32(7.549789954891882e-8)
    r2 = r * r
    s = r + r * r2 * (f32(-1.6666654611e-1) + r2 * (f32(8.3321608736e-3) + r2 * f32(-1.9515295891e-4)))
    c = (1.0 - 0.5 * r2) + r2 * r2 * (
        f32(4.166664568298827e-2) + r2 * (f32(-1.388731625493765e-3) + r2 * f32(2.443315711809948e-5))
    )
    k = n.astype(jnp.int32)
    odd = (k & 1) == 1
    sin_v = jnp.where(odd, c, s)
    cos_v = jnp.where(odd, s, c)
    sin_v = jnp.where((k & 2) == 2, -sin_v, sin_v)
    cos_v = jnp.where(((k + 1) & 2) == 2, -cos_v, cos_v)
    return cos_v, sin_v


def row_max(s3):
    n = s3.shape[0]
    parts = [jnp.max(s3[i * n // 4 : (i + 1) * n // 4], axis=0) for i in range(4)]
    mx = jnp.maximum(jnp.maximum(parts[0], parts[1]), jnp.maximum(parts[2], parts[3]))
    mx = jnp.maximum(mx, pltpu.roll(mx, 4, 0))
    mx = jnp.maximum(mx, pltpu.roll(mx, 2, 0))
    return jnp.maximum(mx, pltpu.roll(mx, 1, 0))


def kernel(
    n_ctx,
    bq_hbm, bk_hbm, bv_hbm, fq_hbm, fk_hbm, fv_hbm, seg_hbm, pos_hbm, w_hbm,
    band_out, proj_out,
    bq_ref, bk_ref, bv_ref, fq_ref, fk_ref, fv_ref, seg_ref, pos_ref,
    kvt, seg_all, kp, qf, qb, bkt, halo, halo_seg, bkp, bias_f, bias_b, m_s, acc, mixed, wv, wt,
    part, rp, snd, rbuf, fin, keep,
    in_sem, z_send, y_send, kv_recv, halo_send, halo_recv, p_send, p_recv, x_send, x_recv,
):
    ctx = lax.axis_index("ctx")
    head = lax.axis_index("head")
    y = lax.rem(ctx, NY)
    z = ctx // NY
    n_z = n_ctx // NY
    core = lax.rem(head, 2)

    ys = [ctx - y + lax.rem(y + d, NY) for d in (1, 2, 3)]
    xs = [lax.rem(head + 2 * d, 2 * NX) for d in (1, 2, 3)]
    partner = head + 1 - 2 * core

    loads = [
        pltpu.make_async_copy(src, dst, in_sem.at[i])
        for i, (src, dst) in enumerate((
            (fk_hbm, fk_ref), (pos_hbm, pos_ref), (fv_hbm, fv_ref), (seg_hbm, seg_ref), (bk_hbm, bk_ref),
            (bv_hbm, bv_ref), (fq_hbm, fq_ref), (bq_hbm, bq_ref), (w_hbm, wv)))
    ]
    for c in loads:
        c.start()

    def greet(where):
        pl.semaphore_signal(pltpu.get_barrier_semaphore(), inc=1, device_id=where, device_id_type=MESH)

    for c in ys:
        greet({"ctx": c})
    for h in (*xs, partner):
        greet({"head": h})
    met = jnp.int32(7)
    for there, c in ((z > 0, ctx - NY), (z < n_z - 1, ctx + NY), (ctx > 0, ctx - 1), (ctx < n_ctx - 1, ctx + 1)):
        pl.when(there)(lambda c=c: greet({"ctx": c}))
        met = met + there.astype(jnp.int32)

    own = 3 * NY

    def present(k, d):
        if k < 3:
            return z >= k
        return z >= 3 if d == 0 else (y >= d) | (z >= 3)

    for k in (1, 2, 3):
        for d in range(NY):
            @pl.when(jnp.logical_not(present(k, d)))
            def _(slot=4 * (k - 1) + d):
                kvt[slot, 0:128, :] = jnp.zeros((128, T), bf16)
                seg_all[slot] = jnp.full((1, T), -1, jnp.int32)

    @pl.when(ctx == 0)
    def _():
        halo[...] = jnp.zeros((128, 128), bf16)
        halo_seg[...] = jnp.full((1, 128), -1, jnp.int32)

    ones16 = jnp.ones((16, T), bf16)
    for i in range(own + 1):
        kvt[i, 128:144, :] = ones16
    bkt[128:144, :] = ones16
    fi = lax.broadcasted_iota(jnp.int32, (HALF, T), 0)
    freq = jnp.ones((HALF, T), f32)
    for i in range(1, HALF):
        freq = jnp.where(fi == i, f32(np.float32(THETA ** (-2.0 * i / HEAD_DIM))), freq)

    loads[0].wait()
    loads[1].wait()
    pos = pos_ref[...].astype(f32)
    cosine, sine = cos_sin(freq * pos)
    cos_q, sin_q = cosine * f32(Q_SCALE), sine * f32(Q_SCALE)

    def rotated(xt, c, s):
        a = xt[0:HALF].astype(f32)
        b = xt[HALF : 2 * HALF].astype(f32)
        return (a * c - b * s).astype(bf16), (b * c + a * s).astype(bf16)

    def store_kv(dst, k_ref, v_ref):
        lo, hi = rotated(k_ref[...], cosine, sine)
        dst[0:HALF, :] = lo
        dst[HALF : 2 * HALF, :] = hi
        dst[64:128, :] = v_ref[...]

    for c in loads[2:6]:
        c.wait()
    store_kv(kvt.at[own], fk_ref, fv_ref)
    store_kv(bkt, bk_ref, bv_ref)
    seg_row = seg_ref[...]
    seg_all[own] = seg_row

    pl.semaphore_wait(pltpu.get_barrier_semaphore(), met)

    K_ROWS, V_ROWS, SEG = 0, 1, 2

    def piece(slot, i):
        return seg_all.at[slot] if i == SEG else kvt.at[slot, pl.ds(64 * i, 64)]

    def send(src_slot, dst_slot, i, ssem, where):
        return pltpu.make_async_remote_copy(
            src_ref=piece(src_slot, i), dst_ref=piece(dst_slot, i), send_sem=ssem, recv_sem=kv_recv.at[dst_slot, i],
            device_id={"ctx": where}, device_id_type=MESH)

    def slot_of(k, d):
        return own if k == 0 else 4 * (k - 1) + d

    def z_copy(k, i):
        return send(slot_of(k, 0), slot_of(k + 1, 0), i, z_send.at[k, i], ctx + NY)

    def z_guard(k):
        return (z >= k) & (z < n_z - 1)

    def z_start(k, i):
        pl.when(z_guard(k))(lambda: z_copy(k, i).start())

    def y_copy(k, d, i):
        if k in (1, 2) and d == 2:
            via, to = (3, 2) if i == V_ROWS else (1, 0)
            return send(slot_of(k, via), slot_of(k, 2), i, y_send.at[k, 1, i], ys[to])
        return send(slot_of(k, 0), slot_of(k or 3, d), i, y_send.at[k, d - 1, i], ys[d - 1])

    def y_guard(k, d):
        if k == 0:
            return y + d < NY
        if k == 3:
            return (y + d >= NY) & (z >= 3)
        return z >= k

    def y_start(k, d, i):
        pl.when(y_guard(k, d))(lambda: y_copy(k, d, i).start())

    def recv(slot, i):
        ref = piece(slot, i)
        pltpu.make_async_remote_copy(
            src_ref=ref, dst_ref=ref, send_sem=z_send.at[0, 0], recv_sem=kv_recv.at[slot, i],
            device_id={"head": partner}, device_id_type=MESH).wait_recv()

    def arrive(k, d, i):
        pl.when(present(k, d))(lambda: recv(slot_of(k, d), i))

    rim = pl.ds(T - WINDOW, WINDOW)
    halo_copies = [
        pltpu.make_async_remote_copy(
            src_ref=src, dst_ref=dst, send_sem=halo_send.at[i], recv_sem=halo_recv.at[i],
            device_id={"ctx": ctx + 1}, device_id_type=MESH)
        for i, (src, dst) in enumerate((
            (bkt.at[pl.ds(0, 128), rim], halo), (seg_all.at[own, pl.ds(0, 1), rim], halo_seg)))
    ]

    for i in (SEG, K_ROWS, V_ROWS):
        z_start(0, i)

    @pl.when(ctx < n_ctx - 1)
    def _():
        for c in halo_copies:
            c.start()

    for d in (1, 3, 2):
        for i in (SEG, K_ROWS, V_ROWS):
            y_start(0, d, i)

    def relay(k):
        arrive(k, 0, SEG)
        arrive(k, 0, K_ROWS)
        if k < 3:
            z_start(k, SEG)
            z_start(k, K_ROWS)
        y_start(k, 1, SEG)
        y_start(k, 3, SEG)
        y_start(k, 1, K_ROWS)
        arrive(k, 0, V_ROWS)
        if k < 3:
            z_start(k, V_ROWS)
        y_start(k, 3, V_ROWS)
        y_start(k, 1, V_ROWS)
        y_start(k, 3, K_ROWS)
        if k == 3:
            for i in (SEG, K_ROWS, V_ROWS):
                y_start(3, 2, i)

    def across(k):
        arrive(k, 1, SEG)
        arrive(k, 1, K_ROWS)
        y_start(k, 2, SEG)
        y_start(k, 2, K_ROWS)
        arrive(k, 3, V_ROWS)
        y_start(k, 2, V_ROWS)

    seg_f = seg_row.astype(f32)
    seg0 = seg_f[0:1, 0:1]

    def seg_cols(row128):
        return jnp.broadcast_to(row128, (128, 128)).T

    def halves(cols):
        return [jnp.concatenate([c[32 * p + 16 * h : 32 * p + 16 * h + 16] for c in cols for p in range(4)], axis=0) for h in range(2)]

    own_seg_cols = [seg_cols(seg_f[:, h * 128 : (h + 1) * 128]) for h in range(2)]
    pos_cols = [seg_cols(pos[:, h * 128 : (h + 1) * 128]) for h in range(2)]
    seg_p = jnp.concatenate([c.T[0:1] for c in halves(own_seg_cols)], axis=1)
    pos_p = jnp.concatenate([c.T[0:1] for c in halves(pos_cols)], axis=1)
    cos_p, sin_p = cos_sin(freq * pos_p)
    cos_p, sin_p = cos_p * f32(Q_SCALE), sin_p * f32(Q_SCALE)
    row_bias = jnp.where(seg_p == seg0, f32(0), f32(NEG))
    i16 = lax.broadcasted_iota(jnp.int32, (16, T), 0)
    feat = jnp.where(i16 == 0, f32(1), jnp.where(i16 == 1, jnp.broadcast_to(row_bias, (16, T)), f32(0))).astype(bf16)
    zeros48 = jnp.zeros((48, 2048), bf16)
    qf[80:128, :] = zeros48
    qb[80:128, :] = zeros48
    qb[64:80, :] = jnp.zeros((16, 2048), bf16)

    def cols(h, g):
        return slice((h * G + g) * 128, (h * G + g + 1) * 128)

    def prep_q(dst, src, c_q, s_q, split):
        for j in range(G // 2):
            at = slice(j * 128, (j + 1) * 128)
            if split:
                rows = [src[32 * p + 16 * h : 32 * p + 16 * h + 16, at] for h in range(2) for p in range(8)]
                xt = jnp.concatenate(rows, axis=0).T
            else:
                xt = src[:, at].T
            for e in range(2):
                lo, hi = rotated(xt[e * 64 : (e + 1) * 64], c_q, s_q)
                for h in range(2):
                    c = cols(h, 2 * j + e)
                    dst[0:HALF, c] = lo[:, h * 128 : (h + 1) * 128]
                    dst[HALF : 2 * HALF, c] = hi[:, h * 128 : (h + 1) * 128]

    loads[6].wait()
    prep_q(qf, fq_ref, cos_p, sin_p, True)
    for h in range(2):
        for g in range(G):
            qf[64:80, cols(h, g)] = feat[:, h * 128 : (h + 1) * 128]

    def key_rows(kt):
        n = kt.shape[1]
        return jnp.concatenate([kt, jnp.zeros((64, n), bf16)], axis=0).T

    ki = lax.broadcasted_iota(jnp.int32, (128, 128), 0)
    ti = lax.broadcasted_iota(jnp.int32, (128, 128), 1)
    for kh in range(2):
        for h in range(2):
            ok = (own_seg_cols[kh] == seg_p[:, h * 128 : (h + 1) * 128])
            ok = ok & (ki + 128 * kh <= 32 * (ti >> 4) + 16 * h + (ti & 15))
            bias_f[kh * 128 : (kh + 1) * 128, h * 128 : (h + 1) * 128] = jnp.where(ok, f32(0), f32(NEG))

    kp[0:T, :] = key_rows(kvt[own, 0:64, :])

    def run_tiles(tiles, stage_a, stage_b, stage_c, lead=3):
        s, p = {}, {}
        for r in range(min(lead, len(tiles))):
            s[r] = stage_a(*tiles[r])
        for r in range(len(tiles)):
            if r + lead < len(tiles):
                s[r + lead] = stage_a(*tiles[r + lead])
            p[r] = stage_b(*tiles[r], s.pop(r))
            if r >= 1:
                stage_c(*tiles[r - 1], *p.pop(r - 1))
        stage_c(*tiles[-1], *p.pop(len(tiles) - 1))

    tiles = [(h, g) for h in range(2) for g in range(G)]

    def diag_a(h, g):
        return jnp.dot(kp[0:T, :], qf[:, cols(h, g)], preferred_element_type=f32) + bias_f[:, h * 128 : (h + 1) * 128]

    def diag_b(h, g, s):
        s3 = s.reshape(T // 8, 8, 128)
        mn = row_max(s3)
        m_s[:, cols(h, g)] = mn
        return (jnp.exp2(s3 - mn[None]).reshape(T, 128).astype(bf16),)

    def diag_c(h, g, p):
        acc[:, cols(h, g)] = jnp.dot(kvt[own, 64:144, :], p, preferred_element_type=f32)

    run_tiles(tiles, diag_a, diag_b, diag_c)

    loads[8].wait()
    for j in range(0, D, 128):
        n = min(128, D - j)
        wt[:, j : j + n] = wv[j : j + n, :].T

    relay(1)

    def band_layer():
        @pl.when(ctx > 0)
        def _():
            for c in halo_copies:
                c.wait_recv()

        halo_seg_cols = seg_cols(halo_seg[...].astype(f32))
        same_h0 = [halo_seg_cols == seg_f[:, 0:128], own_seg_cols[0] == seg_f[:, 0:128]]
        same_h1 = [own_seg_cols[0] == seg_f[:, 128:256], own_seg_cols[1] == seg_f[:, 128:256]]
        for h, same in enumerate((same_h0, same_h1)):
            bias_b[0:128, h * 128 : (h + 1) * 128] = jnp.where(same[0] & (ki > ti), f32(0), f32(NEG))
            bias_b[128:256, h * 128 : (h + 1) * 128] = jnp.where(same[1] & (ki <= ti), f32(0), f32(NEG))
        bkp[0:128, :] = key_rows(halo[0:64, :])
        bkp[128:384, :] = key_rows(bkt[0:64, :])

        band_t = {}

        def band_a(h, g):
            return jnp.dot(bkp[h * 128 : h * 128 + 256, :], qb[:, cols(h, g)], preferred_element_type=f32) + bias_b[:, h * 128 : (h + 1) * 128]

        def band_b(h, g, s):
            s3 = s.reshape(T // 8, 8, 128)
            mn = row_max(s3)
            return (jnp.exp2(s3 - mn[None]).reshape(T, 128).astype(bf16),)

        def band_c(h, g, p):
            if h == 0:
                vt = jnp.concatenate([
                    jnp.concatenate([halo[64:128, :], jnp.ones((16, 128), bf16)], axis=0), bkt[64:144, 0:128]], axis=1)
            else:
                vt = bkt[64:144, :]
            o = jnp.dot(vt, p, preferred_element_type=f32)
            band_t[h, g] = (o[0:64] * (1.0 / o[64:65])).astype(bf16)
            if g % 2 == 1:
                pair = jnp.concatenate([band_t.pop((h, g - 1)), band_t.pop((h, g))], axis=0)
                band_out[h * 128 : (h + 1) * 128, (g - 1) * 64 : (g + 1) * 64] = pair.T

        run_tiles(tiles, band_a, band_b, band_c)

    def group(members, between=None):
        size = len(members)
        for n, (k, d, pieces) in enumerate(members):
            slot = slot_of(k, d)
            for i in pieces:
                arrive(k, d, i)
            kb = jnp.where(seg_all[slot].astype(f32) == seg0, f32(0), f32(NEG))
            kfeat = jnp.where(i16 == 0, jnp.broadcast_to(kb, (16, T)), jnp.where(i16 == 1, f32(1), f32(0))).astype(bf16)
            full = jnp.concatenate([kvt[slot, 0:64, :], kfeat, jnp.zeros((48, T), bf16)], axis=0)
            kp[n * T : (n + 1) * T, :] = full.T

        def a(h, g):
            return jnp.dot(kp[0 : size * T, :], qf[:, cols(h, g)], preferred_element_type=f32)

        def b(h, g, s):
            s3 = s.reshape(size * T // 8, 8, 128)
            mo = m_s[:, cols(h, g)]
            mn = jnp.maximum(mo, row_max(s3))
            m_s[:, cols(h, g)] = mn
            return jnp.exp2(s3 - mn[None]).reshape(size * T, 128).astype(bf16), jnp.exp2(mo - mn)

        def c(h, g, p, al):
            o = None
            for n, (k, d, _) in enumerate(members):
                t = jnp.dot(kvt[slot_of(k, d), 64:144, :], p[n * T : (n + 1) * T], preferred_element_type=f32)
                o = t if o is None else o + t
            acc[:, cols(h, g)] = (acc[:, cols(h, g)].reshape(10, 8, 128) * al[None]).reshape(80, 128) + o

        if between is None:
            run_tiles(tiles, a, b, c)
        else:
            run_tiles(tiles[:G], a, b, c)
            between()
            run_tiles(tiles[G:], a, b, c)

    every = (SEG, K_ROWS, V_ROWS)
    group(((1, 0, ()),))
    loads[7].wait()
    prep_q(qb, bq_ref, cos_q, sin_q, False)
    relay(2)
    across(1)
    group(((2, 0, ()), (1, 1, (V_ROWS,)), (1, 3, (SEG, K_ROWS))))
    relay(3)
    across(2)
    group(((2, 1, (V_ROWS,)), (2, 3, (SEG, K_ROWS))))
    group(((1, 2, every), (3, 0, ())))

    def p_copy(h, i):
        lo, n = COLS[i]
        at = pl.ds(0, 64), pl.ds(lo, n)
        return pltpu.make_async_remote_copy(
            src_ref=part.at[h, *at], dst_ref=rp.at[h, *at],
            send_sem=p_send.at[h, i], recv_sem=p_recv.at[h, i], device_id={"head": partner}, device_id_type=MESH)

    def project(h):
        for g in range(0, G, 2):
            pair = []
            for e in range(2):
                o = acc[:, cols(h, g + e)]
                pair.append((o[0:64] * (1.0 / o[64:65])).astype(bf16))
            mixed[:, g * 64 : (g + 2) * 64] = jnp.concatenate(pair, axis=0).T
        lhs = jnp.concatenate(
            [mixed[pl.ds(pl.multiple_of(32 * i + 16 * c, 16), 16), :] for c in (1 - core, core) for i in range(NX)], axis=0)
        for i, (lo, n) in enumerate(COLS):
            part[h, :, lo : lo + n] = jnp.dot(lhs, wt[:, lo : lo + n], preferred_element_type=f32).astype(bf16)
            p_copy(h, i).start()

    chip = head // 2
    far, up, down = [lax.rem(chip + d, NX) for d in (2, 1, 3)]
    x_up, x_down = xs[0], xs[2]
    lo_c, hi_c = slice(0, SPLIT), slice(SPLIT, D)
    lo_d, hi_d = pl.ds(0, SPLIT), pl.ds(SPLIT, D - SPLIT)

    def x_copy(h, n):
        src, dst, where = (
            (snd.at[h, 0, :, lo_d], rbuf.at[h, :, lo_d], x_up),
            (snd.at[h, 0, :, hi_d], rbuf.at[h, :, hi_d], x_down),
            (snd.at[h, 1, :, hi_d], fin.at[h, 0, :, hi_d], x_up),
            (snd.at[h, 2, :, lo_d], fin.at[h, 1, :, lo_d], x_down),
            (snd.at[h, 1, :, lo_d], fin.at[h, 0, :, lo_d], x_up),
            (snd.at[h, 2, :, hi_d], fin.at[h, 1, :, hi_d], x_down),
        )[n]
        return pltpu.make_async_remote_copy(
            src_ref=src, dst_ref=dst, send_sem=x_send.at[h, n], recv_sem=x_recv.at[h, n],
            device_id={"head": where}, device_id_type=MESH)

    def pair_sums(h):
        for i in range(len(COLS)):
            p_copy(h, i).wait_recv()

        def chip_sum(i):
            at = pl.ds(pl.multiple_of(16 * i, 16), 16)
            own_at = pl.ds(pl.multiple_of(64 + 16 * i, 16), 16)
            return part[h, own_at, :].astype(f32) + rp[h, at, :].astype(f32)

        snd[h, 0] = chip_sum(far).astype(bf16)
        x_copy(h, 0).start()
        x_copy(h, 1).start()
        s_up = chip_sum(up)
        snd[h, 1, :, hi_c] = s_up[:, hi_c].astype(bf16)
        x_copy(h, 2).start()
        s_down = chip_sum(down)
        snd[h, 2, :, lo_c] = s_down[:, lo_c].astype(bf16)
        x_copy(h, 3).start()
        keep[h, 0] = chip_sum(chip)
        keep[h, 1, :, lo_c] = s_up[:, lo_c]
        keep[h, 1, :, hi_c] = s_down[:, hi_c]

    def pass_sums(h):
        for n, row, at in ((0, 1, lo_c), (1, 2, hi_c)):
            x_copy(h, n).wait_recv()
            snd[h, row, :, at] = (keep[h, 1, :, at] + rbuf[h, :, at].astype(f32)).astype(bf16)
            x_copy(h, 4 + n).start()

    def last_sums(h):
        for n in (2, 3, 4, 5):
            x_copy(h, n).wait_recv()
        proj_out[16 * h : 16 * h + 16, :] = (keep[h, 0] + (fin[h, 0].astype(f32) + fin[h, 1].astype(f32))).astype(bf16)

    group(((2, 2, every), (3, 1, every), (3, 3, every), (3, 2, every)), lambda: project(0))
    pair_sums(0)
    project(1)
    pair_sums(1)
    band_layer()
    pass_sums(0)
    pass_sums(1)
    last_sums(0)
    last_sums(1)

    for i in (SEG, K_ROWS, V_ROWS):
        for k in range(3):
            pl.when(z_guard(k))(lambda: z_copy(k, i).wait_send())
        for k in range(4):
            for d in (1, 2, 3):
                pl.when(y_guard(k, d))(lambda: y_copy(k, d, i).wait_send())

    @pl.when(ctx < n_ctx - 1)
    def _():
        for c in halo_copies:
            c.wait_send()

    for h in range(2):
        for i in range(len(COLS)):
            p_copy(h, i).wait_send()
        for n in range(6):
            x_copy(h, n).wait_send()


def body(n_ctx, bq, bk, bv, fq, fk, fv, seg, pos, w):
    vmem = pl.BlockSpec(memory_space=pltpu.VMEM)
    dma = pltpu.SemaphoreType.DMA
    band, proj = pl.pallas_call(
        functools.partial(kernel, n_ctx),
        out_shape=(jax.ShapeDtypeStruct((T, G * HEAD_DIM), bf16), jax.ShapeDtypeStruct((32, D), bf16)),
        in_specs=[pl.BlockSpec(memory_space=pl.ANY)] * 9,
        out_specs=(vmem, vmem),
        scratch_shapes=[
            pltpu.VMEM((T, 512), bf16),
            pltpu.VMEM((64, T), bf16),
            pltpu.VMEM((64, T), bf16),
            pltpu.VMEM((T, 512), bf16),
            pltpu.VMEM((64, T), bf16),
            pltpu.VMEM((64, T), bf16),
            pltpu.VMEM((1, T), jnp.int32),
            pltpu.VMEM((1, T), jnp.int32),
            pltpu.VMEM((13, 144, T), bf16),
            pltpu.VMEM((13, 1, T), jnp.int32),
            pltpu.VMEM((NY * T, 128), bf16),
            pltpu.VMEM((128, 2048), bf16),
            pltpu.VMEM((128, 2048), bf16),
            pltpu.VMEM((144, T), bf16),
            pltpu.VMEM((128, 128), bf16),
            pltpu.VMEM((1, 128), jnp.int32),
            pltpu.VMEM((384, 128), bf16),
            pltpu.VMEM((T, T), f32),
            pltpu.VMEM((T, T), f32),
            pltpu.VMEM((8, 2048), f32),
            pltpu.VMEM((80, 2048), f32),
            pltpu.VMEM((128, 512), bf16),
            pltpu.VMEM((D, 512), bf16),
            pltpu.VMEM((512, D), bf16),
            pltpu.VMEM((2, 128, D), bf16),
            pltpu.VMEM((2, 64, D), bf16),
            pltpu.VMEM((2, 3, 16, D), bf16),
            pltpu.VMEM((2, 16, D), bf16),
            pltpu.VMEM((2, 2, 16, D), bf16),
            pltpu.VMEM((2, 2, 16, D), f32),
            dma((9,)),
            dma((3, 3)),
            dma((4, 3, 3)),
            dma((12, 3)),
            dma((2,)),
            dma((2,)),
            dma((2, len(COLS))),
            dma((2, len(COLS))),
            dma((2, 6)),
            dma((2, 6)),
        ],
        compiler_params=pltpu.CompilerParams(
            collective_id=0, has_side_effects=True, vmem_limit_bytes=60000 * 1024),
        name="packed_attention",
    )(bq, bk.T, bv.T, fq, fk.T, fv.T, seg.reshape(1, T), pos.reshape(1, T), w.T)

    def hand_over(band_in, proj_in, band_to, proj_to, sems):
        copies = [
            pltpu.make_async_copy(src, dst, sems.at[i])
            for i, (src, dst) in enumerate(((band_in, band_to), (proj_in, proj_to)))
        ]
        for c in copies:
            c.start()
        for c in copies:
            c.wait()

    hbm = pl.BlockSpec(memory_space=pl.ANY)
    return pl.pallas_call(
        hand_over,
        out_shape=(jax.ShapeDtypeStruct((T, G * HEAD_DIM), bf16), jax.ShapeDtypeStruct((32, D), bf16)),
        in_specs=[vmem, vmem],
        out_specs=(hbm, hbm),
        scratch_shapes=[dma((2,))],
        name="hand_over",
    )(band, proj)


def solution(mesh):
    return jax.shard_map(
        functools.partial(body, mesh.shape["ctx"]),
        mesh=mesh,
        in_specs=(
            P("ctx", "head"),
            P("ctx", "head"),
            P("ctx", "head"),
            P("ctx", "head"),
            P("ctx", "head"),
            P("ctx", "head"),
            P("ctx"),
            P("ctx"),
            P("head", None),
        ),
        out_specs=(P("ctx", "head"), P(("ctx", "head"), None)),
        check_vma=False,
    )
```

```python
import functools

import jax
import jax.numpy as jnp
import numpy as np
from jax import lax
from jax.experimental import pallas as pl
from jax.experimental.pallas import tpu as pltpu
from jax.sharding import PartitionSpec as P

f32 = jnp.float32
bf16 = jnp.bfloat16
MESH = pl.DeviceIdType.MESH

HEAD_DIM = 64
HALF = 32
WINDOW = 128
NY = 4
NX = 4
T = 256
G = 8
D = 2880
THETA = 150000.0
NEG = -1e30
Q_SCALE = float(np.log2(np.e) * HEAD_DIM**-0.5)
SPLIT = 1408
COLS = ((0, 1536), (1536, 1344))


def cos_sin(x):
    n = jnp.floor(x * f32(2.0 / np.pi) + 0.5)
    r = ((x - n * f32(1.5703125)) - n * f32(4.837512969970703125e-4)) - n * f32(7.549789954891882e-8)
    r2 = r * r
    s = r + r * r2 * (f32(-1.6666654611e-1) + r2 * (f32(8.3321608736e-3) + r2 * f32(-1.9515295891e-4)))
    c = (1.0 - 0.5 * r2) + r2 * r2 * (
        f32(4.166664568298827e-2) + r2 * (f32(-1.388731625493765e-3) + r2 * f32(2.443315711809948e-5))
    )
    k = n.astype(jnp.int32)
    odd = (k & 1) == 1
    sin_v = jnp.where(odd, c, s)
    cos_v = jnp.where(odd, s, c)
    sin_v = jnp.where((k & 2) == 2, -sin_v, sin_v)
    cos_v = jnp.where(((k + 1) & 2) == 2, -cos_v, cos_v)
    return cos_v, sin_v


def row_max(s3):
    n = s3.shape[0]
    parts = [jnp.max(s3[i * n // 4 : (i + 1) * n // 4], axis=0) for i in range(4)]
    mx = jnp.maximum(jnp.maximum(parts[0], parts[1]), jnp.maximum(parts[2], parts[3]))
    mx = jnp.maximum(mx, pltpu.roll(mx, 4, 0))
    mx = jnp.maximum(mx, pltpu.roll(mx, 2, 0))
    return jnp.maximum(mx, pltpu.roll(mx, 1, 0))


def kernel(
    n_ctx,
    bq_hbm, bk_hbm, bv_hbm, fq_hbm, fk_hbm, fv_hbm, seg_hbm, pos_hbm, w_hbm,
    band_out, proj_out,
    bq_ref, bk_ref, bv_ref, fq_ref, fk_ref, fv_ref, seg_ref, pos_ref,
    kvt, seg_all, kp, qf, qb, bkt, halo, halo_seg, halo_via, halo_via_seg, bkp, bias_f, bias_b, m_s, acc, mixed, wv, wt,
    part, rp, snd, rbuf, fin, keep,
    in_sem, z_send, y_send, kv_recv, halo_send, halo_recv, p_send, p_recv, x_send, x_recv,
):
    ctx = lax.axis_index("ctx")
    head = lax.axis_index("head")
    y = lax.rem(ctx, NY)
    z = ctx // NY
    n_z = n_ctx // NY
    core = lax.rem(head, 2)

    ys = [ctx - y + lax.rem(y + d, NY) for d in (1, 2, 3)]
    xs = [lax.rem(head + 2 * d, 2 * NX) for d in (1, 2, 3)]
    partner = head + 1 - 2 * core

    loads = [
        pltpu.make_async_copy(src, dst, in_sem.at[i])
        for i, (src, dst) in enumerate((
            (fk_hbm, fk_ref), (pos_hbm, pos_ref), (fv_hbm, fv_ref), (seg_hbm, seg_ref), (bk_hbm, bk_ref),
            (bv_hbm, bv_ref), (fq_hbm, fq_ref), (bq_hbm, bq_ref), (w_hbm, wv)))
    ]
    for c in loads:
        c.start()

    def greet(where):
        pl.semaphore_signal(pltpu.get_barrier_semaphore(), inc=1, device_id=where, device_id_type=MESH)

    for c in ys:
        greet({"ctx": c})
    for h in (*xs, partner):
        greet({"head": h})
    met = jnp.int32(7)
    for there, c in ((z > 0, ctx - NY), (z < n_z - 1, ctx + NY)):
        pl.when(there)(lambda c=c: greet({"ctx": c}))
        met = met + there.astype(jnp.int32)

    own = 3 * NY

    def present(k, d):
        if k < 3:
            return z >= k
        return z >= 3 if d == 0 else (y >= d) | (z >= 3)

    for k in (1, 2, 3):
        for d in range(NY):
            @pl.when(jnp.logical_not(present(k, d)))
            def _(slot=4 * (k - 1) + d):
                kvt[slot, 0:128, :] = jnp.zeros((128, T), bf16)
                seg_all[slot] = jnp.full((1, T), -1, jnp.int32)

    @pl.when(ctx == 0)
    def _():
        halo[...] = jnp.zeros((128, 128), bf16)
        halo_seg[...] = jnp.full((1, 128), -1, jnp.int32)

    ones16 = jnp.ones((16, T), bf16)
    for i in range(own + 1):
        kvt[i, 128:144, :] = ones16
    bkt[128:144, :] = ones16
    fi = lax.broadcasted_iota(jnp.int32, (HALF, T), 0)
    freq = jnp.ones((HALF, T), f32)
    for i in range(1, HALF):
        freq = jnp.where(fi == i, f32(np.float32(THETA ** (-2.0 * i / HEAD_DIM))), freq)

    loads[0].wait()
    loads[1].wait()
    pos = pos_ref[...].astype(f32)
    cosine, sine = cos_sin(freq * pos)
    cos_q, sin_q = cosine * f32(Q_SCALE), sine * f32(Q_SCALE)

    def rotated(xt, c, s):
        a = xt[0:HALF].astype(f32)
        b = xt[HALF : 2 * HALF].astype(f32)
        return (a * c - b * s).astype(bf16), (b * c + a * s).astype(bf16)

    def store_kv(dst, k_ref, v_ref):
        lo, hi = rotated(k_ref[...], cosine, sine)
        dst[0:HALF, :] = lo
        dst[HALF : 2 * HALF, :] = hi
        dst[64:128, :] = v_ref[...]

    for c in loads[2:6]:
        c.wait()
    store_kv(kvt.at[own], fk_ref, fv_ref)
    store_kv(bkt, bk_ref, bv_ref)
    seg_row = seg_ref[...]
    seg_all[own] = seg_row

    pl.semaphore_wait(pltpu.get_barrier_semaphore(), met)

    K_ROWS, V_ROWS, SEG = 0, 1, 2

    def piece(slot, i):
        return seg_all.at[slot] if i == SEG else kvt.at[slot, pl.ds(64 * i, 64)]

    def send(src_slot, dst_slot, i, ssem, where):
        return pltpu.make_async_remote_copy(
            src_ref=piece(src_slot, i), dst_ref=piece(dst_slot, i), send_sem=ssem, recv_sem=kv_recv.at[dst_slot, i],
            device_id={"ctx": where}, device_id_type=MESH)

    def slot_of(k, d):
        return own if k == 0 else 4 * (k - 1) + d

    def z_copy(k, i):
        return send(slot_of(k, 0), slot_of(k + 1, 0), i, z_send.at[k, i], ctx + NY)

    def z_guard(k):
        return (z >= k) & (z < n_z - 1)

    def z_start(k, i):
        pl.when(z_guard(k))(lambda: z_copy(k, i).start())

    def y_copy(k, d, i):
        if k in (1, 2) and d == 2:
            via, to = (3, 2) if i == V_ROWS else (1, 0)
            return send(slot_of(k, via), slot_of(k, 2), i, y_send.at[k, 1, i], ys[to])
        return send(slot_of(k, 0), slot_of(k or 3, d), i, y_send.at[k, d - 1, i], ys[d - 1])

    def y_guard(k, d):
        if k == 0:
            return y + d < NY
        if k == 3:
            return (y + d >= NY) & (z >= 3)
        return z >= k

    def y_start(k, d, i):
        pl.when(y_guard(k, d))(lambda: y_copy(k, d, i).start())

    def recv(slot, i):
        ref = piece(slot, i)
        pltpu.make_async_remote_copy(
            src_ref=ref, dst_ref=ref, send_sem=z_send.at[0, 0], recv_sem=kv_recv.at[slot, i],
            device_id={"head": partner}, device_id_type=MESH).wait_recv()

    def arrive(k, d, i):
        pl.when(present(k, d))(lambda: recv(slot_of(k, d), i))

    rim = pl.ds(T - WINDOW, WINDOW)
    edge = y == NY - 1

    def halo_copy(n, i):
        src = ((bkt.at[pl.ds(0, 128), rim], seg_all.at[own, pl.ds(0, 1), rim]), (halo_via, halo_via_seg))[n == 2][i]
        dst = ((halo, halo_seg), (halo_via, halo_via_seg))[n == 1][i]
        return pltpu.make_async_remote_copy(
            src_ref=src, dst_ref=dst, send_sem=halo_send.at[n, i], recv_sem=halo_recv.at[int(n == 1), i],
            device_id={"ctx": ctx + NY if n == 1 else ys[0]}, device_id_type=MESH)

    halo_guards = (jnp.logical_not(edge), edge & (z < n_z - 1), edge & (z > 0))

    def halo_start(n):
        @pl.when(halo_guards[n])
        def _():
            for i in range(2):
                halo_copy(n, i).start()

    for i in (SEG, K_ROWS, V_ROWS):
        z_start(0, i)

    halo_start(0)
    halo_start(1)

    for d in (1, 3, 2):
        for i in (SEG, K_ROWS, V_ROWS):
            y_start(0, d, i)

    def relay(k):
        arrive(k, 0, SEG)
        arrive(k, 0, K_ROWS)
        if k < 3:
            z_start(k, SEG)
            z_start(k, K_ROWS)
        y_start(k, 1, SEG)
        y_start(k, 3, SEG)
        y_start(k, 1, K_ROWS)
        arrive(k, 0, V_ROWS)
        if k < 3:
            z_start(k, V_ROWS)
        y_start(k, 3, V_ROWS)
        y_start(k, 1, V_ROWS)
        y_start(k, 3, K_ROWS)
        if k == 3:
            for i in (SEG, K_ROWS, V_ROWS):
                y_start(3, 2, i)

    def across(k):
        arrive(k, 1, SEG)
        arrive(k, 1, K_ROWS)
        y_start(k, 2, SEG)
        y_start(k, 2, K_ROWS)
        arrive(k, 3, V_ROWS)
        y_start(k, 2, V_ROWS)

    seg_f = seg_row.astype(f32)
    seg0 = seg_f[0:1, 0:1]

    def seg_cols(row128):
        return jnp.broadcast_to(row128, (128, 128)).T

    def halves(cols):
        return [jnp.concatenate([c[32 * p + 16 * h : 32 * p + 16 * h + 16] for c in cols for p in range(4)], axis=0) for h in range(2)]

    own_seg_cols = [seg_cols(seg_f[:, h * 128 : (h + 1) * 128]) for h in range(2)]
    pos_cols = [seg_cols(pos[:, h * 128 : (h + 1) * 128]) for h in range(2)]
    seg_p = jnp.concatenate([c.T[0:1] for c in halves(own_seg_cols)], axis=1)
    pos_p = jnp.concatenate([c.T[0:1] for c in halves(pos_cols)], axis=1)
    cos_p, sin_p = cos_sin(freq * pos_p)
    cos_p, sin_p = cos_p * f32(Q_SCALE), sin_p * f32(Q_SCALE)
    row_bias = jnp.where(seg_p == seg0, f32(0), f32(NEG))
    i16 = lax.broadcasted_iota(jnp.int32, (16, T), 0)
    feat = jnp.where(i16 == 0, f32(1), jnp.where(i16 == 1, jnp.broadcast_to(row_bias, (16, T)), f32(0))).astype(bf16)
    zeros48 = jnp.zeros((48, 2048), bf16)
    qf[80:128, :] = zeros48
    qb[80:128, :] = zeros48
    qb[64:80, :] = jnp.zeros((16, 2048), bf16)

    def cols(h, g):
        return slice((h * G + g) * 128, (h * G + g + 1) * 128)

    def prep_q(dst, src, c_q, s_q, split):
        for j in range(G // 2):
            at = slice(j * 128, (j + 1) * 128)
            if split:
                rows = [src[32 * p + 16 * h : 32 * p + 16 * h + 16, at] for h in range(2) for p in range(8)]
                xt = jnp.concatenate(rows, axis=0).T
            else:
                xt = src[:, at].T
            for e in range(2):
                lo, hi = rotated(xt[e * 64 : (e + 1) * 64], c_q, s_q)
                for h in range(2):
                    c = cols(h, 2 * j + e)
                    dst[0:HALF, c] = lo[:, h * 128 : (h + 1) * 128]
                    dst[HALF : 2 * HALF, c] = hi[:, h * 128 : (h + 1) * 128]

    loads[6].wait()
    prep_q(qf, fq_ref, cos_p, sin_p, True)
    for h in range(2):
        for g in range(G):
            qf[64:80, cols(h, g)] = feat[:, h * 128 : (h + 1) * 128]

    def key_rows(kt):
        n = kt.shape[1]
        return jnp.concatenate([kt, jnp.zeros((64, n), bf16)], axis=0).T

    ki = lax.broadcasted_iota(jnp.int32, (128, 128), 0)
    ti = lax.broadcasted_iota(jnp.int32, (128, 128), 1)
    for kh in range(2):
        for h in range(2):
            ok = (own_seg_cols[kh] == seg_p[:, h * 128 : (h + 1) * 128])
            ok = ok & (ki + 128 * kh <= 32 * (ti >> 4) + 16 * h + (ti & 15))
            bias_f[kh * 128 : (kh + 1) * 128, h * 128 : (h + 1) * 128] = jnp.where(ok, f32(0), f32(NEG))

    kp[0:T, :] = key_rows(kvt[own, 0:64, :])

    def run_tiles(tiles, stage_a, stage_b, stage_c, lead=3):
        s, p = {}, {}
        for r in range(min(lead, len(tiles))):
            s[r] = stage_a(*tiles[r])
        for r in range(len(tiles)):
            if r + lead < len(tiles):
                s[r + lead] = stage_a(*tiles[r + lead])
            p[r] = stage_b(*tiles[r], s.pop(r))
            if r >= 1:
                stage_c(*tiles[r - 1], *p.pop(r - 1))
        stage_c(*tiles[-1], *p.pop(len(tiles) - 1))

    tiles = [(h, g) for h in range(2) for g in range(G)]

    def diag_a(h, g):
        return jnp.dot(kp[0:T, :], qf[:, cols(h, g)], preferred_element_type=f32) + bias_f[:, h * 128 : (h + 1) * 128]

    def diag_b(h, g, s):
        s3 = s.reshape(T // 8, 8, 128)
        mn = row_max(s3)
        m_s[:, cols(h, g)] = mn
        return (jnp.exp2(s3 - mn[None]).reshape(T, 128).astype(bf16),)

    def diag_c(h, g, p):
        acc[:, cols(h, g)] = jnp.dot(kvt[own, 64:144, :], p, preferred_element_type=f32)

    run_tiles(tiles, diag_a, diag_b, diag_c)

    loads[8].wait()
    for j in range(0, D, 128):
        n = min(128, D - j)
        wt[:, j : j + n] = wv[j : j + n, :].T

    relay(1)

    def band_layer():
        @pl.when(ctx > 0)
        def _():
            for i in range(2):
                halo_copy(0, i).wait_recv()

        halo_seg_cols = seg_cols(halo_seg[...].astype(f32))
        same_h0 = [halo_seg_cols == seg_f[:, 0:128], own_seg_cols[0] == seg_f[:, 0:128]]
        same_h1 = [own_seg_cols[0] == seg_f[:, 128:256], own_seg_cols[1] == seg_f[:, 128:256]]
        for h, same in enumerate((same_h0, same_h1)):
            bias_b[0:128, h * 128 : (h + 1) * 128] = jnp.where(same[0] & (ki > ti), f32(0), f32(NEG))
            bias_b[128:256, h * 128 : (h + 1) * 128] = jnp.where(same[1] & (ki <= ti), f32(0), f32(NEG))
        bkp[0:128, :] = key_rows(halo[0:64, :])
        bkp[128:384, :] = key_rows(bkt[0:64, :])

        band_t = {}

        def band_a(h, g):
            return jnp.dot(bkp[h * 128 : h * 128 + 256, :], qb[:, cols(h, g)], preferred_element_type=f32) + bias_b[:, h * 128 : (h + 1) * 128]

        def band_b(h, g, s):
            s3 = s.reshape(T // 8, 8, 128)
            mn = row_max(s3)
            return (jnp.exp2(s3 - mn[None]).reshape(T, 128).astype(bf16),)

        def band_c(h, g, p):
            if h == 0:
                vt = jnp.concatenate([
                    jnp.concatenate([halo[64:128, :], jnp.ones((16, 128), bf16)], axis=0), bkt[64:144, 0:128]], axis=1)
            else:
                vt = bkt[64:144, :]
            o = jnp.dot(vt, p, preferred_element_type=f32)
            band_t[h, g] = (o[0:64] * (1.0 / o[64:65])).astype(bf16)
            if g % 2 == 1:
                pair = jnp.concatenate([band_t.pop((h, g - 1)), band_t.pop((h, g))], axis=0)
                band_out[h * 128 : (h + 1) * 128, (g - 1) * 64 : (g + 1) * 64] = pair.T

        run_tiles(tiles, band_a, band_b, band_c)

    def group(members, between=None):
        size = len(members)
        for n, (k, d, pieces) in enumerate(members):
            slot = slot_of(k, d)
            for i in pieces:
                arrive(k, d, i)
            kb = jnp.where(seg_all[slot].astype(f32) == seg0, f32(0), f32(NEG))
            kfeat = jnp.where(i16 == 0, jnp.broadcast_to(kb, (16, T)), jnp.where(i16 == 1, f32(1), f32(0))).astype(bf16)
            full = jnp.concatenate([kvt[slot, 0:64, :], kfeat, jnp.zeros((48, T), bf16)], axis=0)
            kp[n * T : (n + 1) * T, :] = full.T

        def a(h, g):
            return jnp.dot(kp[0 : size * T, :], qf[:, cols(h, g)], preferred_element_type=f32)

        def b(h, g, s):
            s3 = s.reshape(size * T // 8, 8, 128)
            mo = m_s[:, cols(h, g)]
            mn = jnp.maximum(mo, row_max(s3))
            m_s[:, cols(h, g)] = mn
            return jnp.exp2(s3 - mn[None]).reshape(size * T, 128).astype(bf16), jnp.exp2(mo - mn)

        def c(h, g, p, al):
            o = None
            for n, (k, d, _) in enumerate(members):
                t = jnp.dot(kvt[slot_of(k, d), 64:144, :], p[n * T : (n + 1) * T], preferred_element_type=f32)
                o = t if o is None else o + t
            acc[:, cols(h, g)] = (acc[:, cols(h, g)].reshape(10, 8, 128) * al[None]).reshape(80, 128) + o

        if between is None:
            run_tiles(tiles, a, b, c)
        else:
            run_tiles(tiles[:G], a, b, c)
            between[0]()
            run_tiles(tiles[G : G + G // 2], a, b, c)
            between[1]()
            run_tiles(tiles[G + G // 2 :], a, b, c)

    every = (SEG, K_ROWS, V_ROWS)
    group(((1, 0, ()),))
    loads[7].wait()
    prep_q(qb, bq_ref, cos_q, sin_q, False)
    relay(2)
    across(1)

    @pl.when(halo_guards[2])
    def _():
        for i in range(2):
            halo_copy(1, i).wait_recv()

    halo_start(2)
    group(((2, 0, ()), (1, 1, (V_ROWS,)), (1, 3, (SEG, K_ROWS))))
    relay(3)
    across(2)
    group(((2, 1, (V_ROWS,)), (2, 3, (SEG, K_ROWS))))
    group(((1, 2, every), (3, 0, ())))

    def p_copy(h, i):
        lo, n = COLS[i]
        at = pl.ds(0, 64), pl.ds(lo, n)
        return pltpu.make_async_remote_copy(
            src_ref=part.at[h, *at], dst_ref=rp.at[h, *at],
            send_sem=p_send.at[h, i], recv_sem=p_recv.at[h, i], device_id={"head": partner}, device_id_type=MESH)

    def project(h):
        for g in range(0, G, 2):
            pair = []
            for e in range(2):
                o = acc[:, cols(h, g + e)]
                pair.append((o[0:64] * (1.0 / o[64:65])).astype(bf16))
            mixed[:, g * 64 : (g + 2) * 64] = jnp.concatenate(pair, axis=0).T
        lhs = jnp.concatenate(
            [mixed[pl.ds(pl.multiple_of(32 * i + 16 * c, 16), 16), :] for c in (1 - core, core) for i in range(NX)], axis=0)
        for i, (lo, n) in enumerate(COLS):
            part[h, :, lo : lo + n] = jnp.dot(lhs, wt[:, lo : lo + n], preferred_element_type=f32).astype(bf16)
            p_copy(h, i).start()

    chip = head // 2
    far, up, down = [lax.rem(chip + d, NX) for d in (2, 1, 3)]
    x_up, x_down = xs[0], xs[2]
    lo_c, hi_c = slice(0, SPLIT), slice(SPLIT, D)
    lo_d, hi_d = pl.ds(0, SPLIT), pl.ds(SPLIT, D - SPLIT)

    def x_copy(h, n):
        src, dst, where = (
            (snd.at[h, 0, :, lo_d], rbuf.at[h, :, lo_d], x_up),
            (snd.at[h, 0, :, hi_d], rbuf.at[h, :, hi_d], x_down),
            (snd.at[h, 1, :, hi_d], fin.at[h, 0, :, hi_d], x_up),
            (snd.at[h, 2, :, lo_d], fin.at[h, 1, :, lo_d], x_down),
            (snd.at[h, 1, :, lo_d], fin.at[h, 0, :, lo_d], x_up),
            (snd.at[h, 2, :, hi_d], fin.at[h, 1, :, hi_d], x_down),
        )[n]
        return pltpu.make_async_remote_copy(
            src_ref=src, dst_ref=dst, send_sem=x_send.at[h, n], recv_sem=x_recv.at[h, n],
            device_id={"head": where}, device_id_type=MESH)

    def pair_sums(h):
        for i in range(len(COLS)):
            p_copy(h, i).wait_recv()

        def chip_sum(i):
            at = pl.ds(pl.multiple_of(16 * i, 16), 16)
            own_at = pl.ds(pl.multiple_of(64 + 16 * i, 16), 16)
            return part[h, own_at, :].astype(f32) + rp[h, at, :].astype(f32)

        snd[h, 0] = chip_sum(far).astype(bf16)
        x_copy(h, 0).start()
        x_copy(h, 1).start()
        s_up = chip_sum(up)
        snd[h, 1, :, hi_c] = s_up[:, hi_c].astype(bf16)
        x_copy(h, 2).start()
        s_down = chip_sum(down)
        snd[h, 2, :, lo_c] = s_down[:, lo_c].astype(bf16)
        x_copy(h, 3).start()
        keep[h, 0] = chip_sum(chip)
        keep[h, 1, :, lo_c] = s_up[:, lo_c]
        keep[h, 1, :, hi_c] = s_down[:, hi_c]

    def pass_sums(h):
        for n, row, at in ((0, 1, lo_c), (1, 2, hi_c)):
            x_copy(h, n).wait_recv()
            snd[h, row, :, at] = (keep[h, 1, :, at] + rbuf[h, :, at].astype(f32)).astype(bf16)
            x_copy(h, 4 + n).start()

    def last_sums(h):
        for n in (2, 3, 4, 5):
            x_copy(h, n).wait_recv()
        proj_out[16 * h : 16 * h + 16, :] = (keep[h, 0] + (fin[h, 0].astype(f32) + fin[h, 1].astype(f32))).astype(bf16)

    group(((2, 2, every), (3, 1, every), (3, 3, every), (3, 2, every)), (lambda: project(0), lambda: pair_sums(0)))
    project(1)
    band_layer()
    pair_sums(1)
    pass_sums(0)
    pass_sums(1)
    last_sums(0)
    last_sums(1)

    for i in (SEG, K_ROWS, V_ROWS):
        for k in range(3):
            pl.when(z_guard(k))(lambda: z_copy(k, i).wait_send())
        for k in range(4):
            for d in (1, 2, 3):
                pl.when(y_guard(k, d))(lambda: y_copy(k, d, i).wait_send())

    for n in range(3):
        @pl.when(halo_guards[n])
        def _(n=n):
            for i in range(2):
                halo_copy(n, i).wait_send()

    for h in range(2):
        for i in range(len(COLS)):
            p_copy(h, i).wait_send()
        for n in range(6):
            x_copy(h, n).wait_send()


def body(n_ctx, bq, bk, bv, fq, fk, fv, seg, pos, w):
    vmem = pl.BlockSpec(memory_space=pltpu.VMEM)
    dma = pltpu.SemaphoreType.DMA
    band, proj = pl.pallas_call(
        functools.partial(kernel, n_ctx),
        out_shape=(pltpu.VMEM((T, G * HEAD_DIM), bf16), pltpu.VMEM((32, D), bf16)),
        in_specs=[pl.BlockSpec(memory_space=pl.ANY)] * 9,
        out_specs=(vmem, vmem),
        scratch_shapes=[
            pltpu.VMEM((T, 512), bf16),
            pltpu.VMEM((64, T), bf16),
            pltpu.VMEM((64, T), bf16),
            pltpu.VMEM((T, 512), bf16),
            pltpu.VMEM((64, T), bf16),
            pltpu.VMEM((64, T), bf16),
            pltpu.VMEM((1, T), jnp.int32),
            pltpu.VMEM((1, T), jnp.int32),
            pltpu.VMEM((13, 144, T), bf16),
            pltpu.VMEM((13, 1, T), jnp.int32),
            pltpu.VMEM((NY * T, 128), bf16),
            pltpu.VMEM((128, 2048), bf16),
            pltpu.VMEM((128, 2048), bf16),
            pltpu.VMEM((144, T), bf16),
            pltpu.VMEM((128, 128), bf16),
            pltpu.VMEM((1, 128), jnp.int32),
            pltpu.VMEM((128, 128), bf16),
            pltpu.VMEM((1, 128), jnp.int32),
            pltpu.VMEM((384, 128), bf16),
            pltpu.VMEM((T, T), f32),
            pltpu.VMEM((T, T), f32),
            pltpu.VMEM((8, 2048), f32),
            pltpu.VMEM((80, 2048), f32),
            pltpu.VMEM((128, 512), bf16),
            pltpu.VMEM((D, 512), bf16),
            pltpu.VMEM((512, D), bf16),
            pltpu.VMEM((2, 128, D), bf16),
            pltpu.VMEM((2, 64, D), bf16),
            pltpu.VMEM((2, 3, 16, D), bf16),
            pltpu.VMEM((2, 16, D), bf16),
            pltpu.VMEM((2, 2, 16, D), bf16),
            pltpu.VMEM((2, 2, 16, D), f32),
            dma((9,)),
            dma((3, 3)),
            dma((4, 3, 3)),
            dma((12, 3)),
            dma((3, 2)),
            dma((2, 2)),
            dma((2, len(COLS))),
            dma((2, len(COLS))),
            dma((2, 6)),
            dma((2, 6)),
        ],
        compiler_params=pltpu.CompilerParams(
            collective_id=0, has_side_effects=True, vmem_limit_bytes=60000 * 1024),
        name="packed_attention",
    )(bq, bk.T, bv.T, fq, fk.T, fv.T, seg.reshape(1, T), pos.reshape(1, T), w.T)

    def hand_over(band_in, proj_in, band_to, proj_to, sems):
        copies = [
            pltpu.make_async_copy(src, dst, sems.at[i])
            for i, (src, dst) in enumerate(((band_in, band_to), (proj_in, proj_to)))
        ]
        for c in copies:
            c.start()
        for c in copies:
            c.wait()

    hbm = pl.BlockSpec(memory_space=pl.ANY)
    return pl.pallas_call(
        hand_over,
        out_shape=(jax.ShapeDtypeStruct((T, G * HEAD_DIM), bf16), jax.ShapeDtypeStruct((32, D), bf16)),
        in_specs=[hbm, hbm],
        out_specs=(hbm, hbm),
        scratch_shapes=[dma((2,))],
        compiler_params=pltpu.CompilerParams(vmem_limit_bytes=1024 * 1024),
        name="hand_over",
    )(band, proj)


def solution(mesh):
    return jax.shard_map(
        functools.partial(body, mesh.shape["ctx"]),
        mesh=mesh,
        in_specs=(
            P("ctx", "head"),
            P("ctx", "head"),
            P("ctx", "head"),
            P("ctx", "head"),
            P("ctx", "head"),
            P("ctx", "head"),
            P("ctx"),
            P("ctx"),
            P("head", None),
        ),
        out_specs=(P("ctx", "head"), P(("ctx", "head"), None)),
        check_vma=False,
    )
```

```python
import functools

import jax
import jax.numpy as jnp
import numpy as np
from jax import lax
from jax.experimental import pallas as pl
from jax.experimental.pallas import tpu as pltpu
from jax.sharding import PartitionSpec as P

f32 = jnp.float32
bf16 = jnp.bfloat16
MESH = pl.DeviceIdType.MESH

HEAD_DIM = 64
HALF = 32
WINDOW = 128
NY = 4
NX = 4
T = 256
G = 8
D = 2880
THETA = 150000.0
NEG = -1e30
Q_SCALE = float(np.log2(np.e) * HEAD_DIM**-0.5)
SPLIT = 1408
COLS = ((0, 1536), (1536, 1344))


def cos_sin(x):
    n = jnp.floor(x * f32(2.0 / np.pi) + 0.5)
    r = ((x - n * f32(1.5703125)) - n * f32(4.837512969970703125e-4)) - n * f32(7.549789954891882e-8)
    r2 = r * r
    s = r + r * r2 * (f32(-1.6666654611e-1) + r2 * (f32(8.3321608736e-3) + r2 * f32(-1.9515295891e-4)))
    c = (1.0 - 0.5 * r2) + r2 * r2 * (
        f32(4.166664568298827e-2) + r2 * (f32(-1.388731625493765e-3) + r2 * f32(2.443315711809948e-5))
    )
    k = n.astype(jnp.int32)
    odd = (k & 1) == 1
    sin_v = jnp.where(odd, c, s)
    cos_v = jnp.where(odd, s, c)
    sin_v = jnp.where((k & 2) == 2, -sin_v, sin_v)
    cos_v = jnp.where(((k + 1) & 2) == 2, -cos_v, cos_v)
    return cos_v, sin_v


def row_max(s3):
    n = s3.shape[0]
    parts = [jnp.max(s3[i * n // 4 : (i + 1) * n // 4], axis=0) for i in range(4)]
    mx = jnp.maximum(jnp.maximum(parts[0], parts[1]), jnp.maximum(parts[2], parts[3]))
    mx = jnp.maximum(mx, pltpu.roll(mx, 4, 0))
    mx = jnp.maximum(mx, pltpu.roll(mx, 2, 0))
    return jnp.maximum(mx, pltpu.roll(mx, 1, 0))


def kernel(
    n_ctx,
    bq_hbm, bk_hbm, bv_hbm, fq_hbm, fk_hbm, fv_hbm, seg_hbm, pos_hbm, w_hbm,
    band_out, proj_out,
    bq_ref, bk_ref, bv_ref, fq_ref, fk_ref, fv_ref, seg_ref, pos_ref,
    kvt, seg_all, kp, qf, qb, bkt, halo, halo_seg, halo_via, halo_via_seg, bkp, bias_f, bias_b, m_s, acc, mixed, wv, wt,
    part, rp, snd, rbuf, fin, keep,
    in_sem, z_send, y_send, kv_recv, halo_send, halo_recv, p_send, p_recv, x_send, x_recv,
):
    ctx = lax.axis_index("ctx")
    head = lax.axis_index("head")
    y = lax.rem(ctx, NY)
    z = ctx // NY
    n_z = n_ctx // NY
    core = lax.rem(head, 2)

    ys = [ctx - y + lax.rem(y + d, NY) for d in (1, 2, 3)]
    xs = [lax.rem(head + 2 * d, 2 * NX) for d in (1, 2, 3)]
    partner = head + 1 - 2 * core

    loads = [
        pltpu.make_async_copy(src, dst, in_sem.at[i])
        for i, (src, dst) in enumerate((
            (fk_hbm, fk_ref), (pos_hbm, pos_ref), (fv_hbm, fv_ref), (seg_hbm, seg_ref), (bk_hbm, bk_ref),
            (bv_hbm, bv_ref), (fq_hbm, fq_ref), (bq_hbm, bq_ref), (w_hbm, wv)))
    ]
    for c in loads:
        c.start()

    def greet(where):
        pl.semaphore_signal(pltpu.get_barrier_semaphore(), inc=1, device_id=where, device_id_type=MESH)

    for c in ys:
        greet({"ctx": c})
    for h in (*xs, partner):
        greet({"head": h})
    met = jnp.int32(7)
    for there, c in ((z > 0, ctx - NY), (z < n_z - 1, ctx + NY)):
        pl.when(there)(lambda c=c: greet({"ctx": c}))
        met = met + there.astype(jnp.int32)

    own = 3 * NY

    def present(k, d):
        if k < 3:
            return z >= k
        return z >= 3 if d == 0 else (y >= d) | (z >= 3)

    for k in (1, 2, 3):
        for d in range(NY):
            @pl.when(jnp.logical_not(present(k, d)))
            def _(slot=4 * (k - 1) + d):
                kvt[slot, 0:128, :] = jnp.zeros((128, T), bf16)
                seg_all[slot] = jnp.full((1, T), -1, jnp.int32)

    @pl.when(ctx == 0)
    def _():
        halo[...] = jnp.zeros((128, 128), bf16)
        halo_seg[...] = jnp.full((1, 128), -1, jnp.int32)

    ones16 = jnp.ones((16, T), bf16)
    for i in range(own + 1):
        kvt[i, 128:144, :] = ones16
    bkt[128:144, :] = ones16
    fi = lax.broadcasted_iota(jnp.int32, (HALF, T), 0)
    freq = jnp.ones((HALF, T), f32)
    for i in range(1, HALF):
        freq = jnp.where(fi == i, f32(np.float32(THETA ** (-2.0 * i / HEAD_DIM))), freq)

    loads[0].wait()
    loads[1].wait()
    pos = pos_ref[...].astype(f32)
    cosine, sine = cos_sin(freq * pos)
    cos_q, sin_q = cosine * f32(Q_SCALE), sine * f32(Q_SCALE)

    def rotated(xt, c, s):
        a = xt[0:HALF].astype(f32)
        b = xt[HALF : 2 * HALF].astype(f32)
        return (a * c - b * s).astype(bf16), (b * c + a * s).astype(bf16)

    def store_kv(dst, k_ref, v_ref):
        lo, hi = rotated(k_ref[...], cosine, sine)
        dst[0:HALF, :] = lo
        dst[HALF : 2 * HALF, :] = hi
        dst[64:128, :] = v_ref[...]

    for c in loads[2:6]:
        c.wait()
    store_kv(kvt.at[own], fk_ref, fv_ref)
    store_kv(bkt, bk_ref, bv_ref)
    seg_row = seg_ref[...]
    seg_all[own] = seg_row

    pl.semaphore_wait(pltpu.get_barrier_semaphore(), met)

    K_ROWS, V_ROWS, SEG = 0, 1, 2

    def piece(slot, i):
        return seg_all.at[slot] if i == SEG else kvt.at[slot, pl.ds(64 * i, 64)]

    def send(src_slot, dst_slot, i, ssem, where):
        return pltpu.make_async_remote_copy(
            src_ref=piece(src_slot, i), dst_ref=piece(dst_slot, i), send_sem=ssem, recv_sem=kv_recv.at[dst_slot, i],
            device_id={"ctx": where}, device_id_type=MESH)

    def slot_of(k, d):
        return own if k == 0 else 4 * (k - 1) + d

    def z_copy(k, i):
        return send(slot_of(k, 0), slot_of(k + 1, 0), i, z_send.at[k, i], ctx + NY)

    def z_guard(k):
        return (z >= k) & (z < n_z - 1)

    def z_start(k, i):
        pl.when(z_guard(k))(lambda: z_copy(k, i).start())

    def y_copy(k, d, i):
        if k in (1, 2) and d == 2:
            via, to = (3, 2) if i == V_ROWS else (1, 0)
            return send(slot_of(k, via), slot_of(k, 2), i, y_send.at[k, 1, i], ys[to])
        return send(slot_of(k, 0), slot_of(k or 3, d), i, y_send.at[k, d - 1, i], ys[d - 1])

    def y_guard(k, d):
        if k == 0:
            return y + d < NY
        if k == 3:
            return (y + d >= NY) & (z >= 3)
        return z >= k

    def y_start(k, d, i):
        pl.when(y_guard(k, d))(lambda: y_copy(k, d, i).start())

    def recv(slot, i):
        ref = piece(slot, i)
        pltpu.make_async_remote_copy(
            src_ref=ref, dst_ref=ref, send_sem=z_send.at[0, 0], recv_sem=kv_recv.at[slot, i],
            device_id={"head": partner}, device_id_type=MESH).wait_recv()

    def arrive(k, d, i):
        pl.when(present(k, d))(lambda: recv(slot_of(k, d), i))

    rim = pl.ds(T - WINDOW, WINDOW)
    edge = y == NY - 1

    def halo_copy(n, i):
        src = ((bkt.at[pl.ds(0, 128), rim], seg_all.at[own, pl.ds(0, 1), rim]), (halo_via, halo_via_seg))[n == 2][i]
        dst = ((halo, halo_seg), (halo_via, halo_via_seg))[n == 1][i]
        return pltpu.make_async_remote_copy(
            src_ref=src, dst_ref=dst, send_sem=halo_send.at[n, i], recv_sem=halo_recv.at[int(n == 1), i],
            device_id={"ctx": ctx + NY if n == 1 else ys[0]}, device_id_type=MESH)

    halo_guards = (jnp.logical_not(edge), edge & (z < n_z - 1), edge & (z > 0))

    def halo_start(n):
        @pl.when(halo_guards[n])
        def _():
            for i in range(2):
                halo_copy(n, i).start()

    for i in (SEG, K_ROWS, V_ROWS):
        z_start(0, i)

    halo_start(0)
    halo_start(1)

    for d in (1, 3, 2):
        for i in (SEG, K_ROWS, V_ROWS):
            y_start(0, d, i)

    def relay(k):
        arrive(k, 0, SEG)
        arrive(k, 0, K_ROWS)
        if k < 3:
            z_start(k, SEG)
            z_start(k, K_ROWS)
        y_start(k, 1, SEG)
        y_start(k, 3, SEG)
        y_start(k, 1, K_ROWS)
        arrive(k, 0, V_ROWS)
        if k < 3:
            z_start(k, V_ROWS)
        y_start(k, 3, V_ROWS)
        y_start(k, 1, V_ROWS)
        y_start(k, 3, K_ROWS)
        if k == 3:
            for i in (SEG, K_ROWS, V_ROWS):
                y_start(3, 2, i)

    def across(k):
        arrive(k, 1, SEG)
        arrive(k, 1, K_ROWS)
        y_start(k, 2, SEG)
        y_start(k, 2, K_ROWS)
        arrive(k, 3, V_ROWS)
        y_start(k, 2, V_ROWS)

    seg_f = seg_row.astype(f32)
    seg0 = seg_f[0:1, 0:1]

    def seg_cols(row128):
        return jnp.broadcast_to(row128, (128, 128)).T

    def halves(cols):
        return [jnp.concatenate([c[32 * p + 16 * h : 32 * p + 16 * h + 16] for c in cols for p in range(4)], axis=0) for h in range(2)]

    own_seg_cols = [seg_cols(seg_f[:, h * 128 : (h + 1) * 128]) for h in range(2)]
    pos_cols = [seg_cols(pos[:, h * 128 : (h + 1) * 128]) for h in range(2)]
    seg_p = jnp.concatenate([c.T[0:1] for c in halves(own_seg_cols)], axis=1)
    pos_p = jnp.concatenate([c.T[0:1] for c in halves(pos_cols)], axis=1)
    cos_p, sin_p = cos_sin(freq * pos_p)
    cos_p, sin_p = cos_p * f32(Q_SCALE), sin_p * f32(Q_SCALE)
    row_bias = jnp.where(seg_p == seg0, f32(0), f32(NEG))
    i16 = lax.broadcasted_iota(jnp.int32, (16, T), 0)
    feat = jnp.where(i16 == 0, f32(1), jnp.where(i16 == 1, jnp.broadcast_to(row_bias, (16, T)), f32(0))).astype(bf16)
    zeros48 = jnp.zeros((48, 2048), bf16)
    qf[80:128, :] = zeros48
    qb[80:128, :] = zeros48
    qb[64:80, :] = jnp.zeros((16, 2048), bf16)

    def cols(h, g):
        return slice((h * G + g) * 128, (h * G + g + 1) * 128)

    def prep_q(dst, src, c_q, s_q, split):
        for j in range(G // 2):
            at = slice(j * 128, (j + 1) * 128)
            if split:
                rows = [src[32 * p + 16 * h : 32 * p + 16 * h + 16, at] for h in range(2) for p in range(8)]
                xt = jnp.concatenate(rows, axis=0).T
            else:
                xt = src[:, at].T
            for e in range(2):
                lo, hi = rotated(xt[e * 64 : (e + 1) * 64], c_q, s_q)
                for h in range(2):
                    c = cols(h, 2 * j + e)
                    dst[0:HALF, c] = lo[:, h * 128 : (h + 1) * 128]
                    dst[HALF : 2 * HALF, c] = hi[:, h * 128 : (h + 1) * 128]

    loads[6].wait()
    prep_q(qf, fq_ref, cos_p, sin_p, True)
    for h in range(2):
        for g in range(G):
            qf[64:80, cols(h, g)] = feat[:, h * 128 : (h + 1) * 128]

    def key_rows(kt):
        n = kt.shape[1]
        return jnp.concatenate([kt, jnp.zeros((64, n), bf16)], axis=0).T

    ki = lax.broadcasted_iota(jnp.int32, (128, 128), 0)
    ti = lax.broadcasted_iota(jnp.int32, (128, 128), 1)
    for kh in range(2):
        for h in range(2):
            ok = (own_seg_cols[kh] == seg_p[:, h * 128 : (h + 1) * 128])
            ok = ok & (ki + 128 * kh <= 32 * (ti >> 4) + 16 * h + (ti & 15))
            bias_f[kh * 128 : (kh + 1) * 128, h * 128 : (h + 1) * 128] = jnp.where(ok, f32(0), f32(NEG))

    kp[0:T, :] = key_rows(kvt[own, 0:64, :])

    def run_tiles(tiles, stage_a, stage_b, stage_c, lead=3):
        s, p = {}, {}
        for r in range(min(lead, len(tiles))):
            s[r] = stage_a(*tiles[r])
        for r in range(len(tiles)):
            if r + lead < len(tiles):
                s[r + lead] = stage_a(*tiles[r + lead])
            p[r] = stage_b(*tiles[r], s.pop(r))
            if r >= 1:
                stage_c(*tiles[r - 1], *p.pop(r - 1))
        stage_c(*tiles[-1], *p.pop(len(tiles) - 1))

    tiles = [(h, g) for h in range(2) for g in range(G)]

    def diag_a(h, g):
        return jnp.dot(kp[0:T, :], qf[:, cols(h, g)], preferred_element_type=f32) + bias_f[:, h * 128 : (h + 1) * 128]

    def diag_b(h, g, s):
        s3 = s.reshape(T // 8, 8, 128)
        mn = row_max(s3)
        m_s[:, cols(h, g)] = mn
        return (jnp.exp2(s3 - mn[None]).reshape(T, 128).astype(bf16),)

    def diag_c(h, g, p):
        acc[:, cols(h, g)] = jnp.dot(kvt[own, 64:144, :], p, preferred_element_type=f32)

    run_tiles(tiles, diag_a, diag_b, diag_c)

    loads[8].wait()
    for j in range(0, D, 128):
        n = min(128, D - j)
        wt[:, j : j + n] = wv[j : j + n, :].T

    relay(1)

    def band_layer():
        @pl.when(ctx > 0)
        def _():
            for i in range(2):
                halo_copy(0, i).wait_recv()

        halo_seg_cols = seg_cols(halo_seg[...].astype(f32))
        same_h0 = [halo_seg_cols == seg_f[:, 0:128], own_seg_cols[0] == seg_f[:, 0:128]]
        same_h1 = [own_seg_cols[0] == seg_f[:, 128:256], own_seg_cols[1] == seg_f[:, 128:256]]
        for h, same in enumerate((same_h0, same_h1)):
            bias_b[0:128, h * 128 : (h + 1) * 128] = jnp.where(same[0] & (ki > ti), f32(0), f32(NEG))
            bias_b[128:256, h * 128 : (h + 1) * 128] = jnp.where(same[1] & (ki <= ti), f32(0), f32(NEG))
        bkp[0:128, :] = key_rows(halo[0:64, :])
        bkp[128:384, :] = key_rows(bkt[0:64, :])

        band_t = {}

        def band_a(h, g):
            return jnp.dot(bkp[h * 128 : h * 128 + 256, :], qb[:, cols(h, g)], preferred_element_type=f32) + bias_b[:, h * 128 : (h + 1) * 128]

        def band_b(h, g, s):
            s3 = s.reshape(T // 8, 8, 128)
            mn = row_max(s3)
            return (jnp.exp2(s3 - mn[None]).reshape(T, 128).astype(bf16),)

        def band_c(h, g, p):
            if h == 0:
                vt = jnp.concatenate([
                    jnp.concatenate([halo[64:128, :], jnp.ones((16, 128), bf16)], axis=0), bkt[64:144, 0:128]], axis=1)
            else:
                vt = bkt[64:144, :]
            o = jnp.dot(vt, p, preferred_element_type=f32)
            band_t[h, g] = (o[0:64] * (1.0 / o[64:65])).astype(bf16)
            if g % 2 == 1:
                pair = jnp.concatenate([band_t.pop((h, g - 1)), band_t.pop((h, g))], axis=0)
                band_out[h * 128 : (h + 1) * 128, (g - 1) * 64 : (g + 1) * 64] = pair.T

        run_tiles(tiles, band_a, band_b, band_c)

    def group(members, between=None):
        size = len(members)
        for n, (k, d, pieces) in enumerate(members):
            slot = slot_of(k, d)
            for i in pieces:
                arrive(k, d, i)
            kb = jnp.where(seg_all[slot].astype(f32) == seg0, f32(0), f32(NEG))
            kfeat = jnp.where(i16 == 0, jnp.broadcast_to(kb, (16, T)), jnp.where(i16 == 1, f32(1), f32(0))).astype(bf16)
            full = jnp.concatenate([kvt[slot, 0:64, :], kfeat, jnp.zeros((48, T), bf16)], axis=0)
            kp[n * T : (n + 1) * T, :] = full.T

        def a(h, g):
            return jnp.dot(kp[0 : size * T, :], qf[:, cols(h, g)], preferred_element_type=f32)

        def b(h, g, s):
            s3 = s.reshape(size * T // 8, 8, 128)
            mo = m_s[:, cols(h, g)]
            mn = jnp.maximum(mo, row_max(s3))
            m_s[:, cols(h, g)] = mn
            return jnp.exp2(s3 - mn[None]).reshape(size * T, 128).astype(bf16), jnp.exp2(mo - mn)

        def c(h, g, p, al):
            o = None
            for n, (k, d, _) in enumerate(members):
                t = jnp.dot(kvt[slot_of(k, d), 64:144, :], p[n * T : (n + 1) * T], preferred_element_type=f32)
                o = t if o is None else o + t
            acc[:, cols(h, g)] = (acc[:, cols(h, g)].reshape(10, 8, 128) * al[None]).reshape(80, 128) + o

        if between is None:
            run_tiles(tiles, a, b, c)
        else:
            run_tiles(tiles[:G], a, b, c)
            between[0]()
            run_tiles(tiles[G : G + G // 2], a, b, c)
            between[1]()
            run_tiles(tiles[G + G // 2 :], a, b, c)

    every = (SEG, K_ROWS, V_ROWS)
    group(((1, 0, ()),))
    loads[7].wait()
    prep_q(qb, bq_ref, cos_q, sin_q, False)
    relay(2)
    across(1)

    @pl.when(halo_guards[2])
    def _():
        for i in range(2):
            halo_copy(1, i).wait_recv()

    halo_start(2)
    group(((2, 0, ()), (1, 1, (V_ROWS,)), (1, 3, (SEG, K_ROWS))))
    relay(3)
    across(2)
    group(((2, 1, (V_ROWS,)), (2, 3, (SEG, K_ROWS))))
    group(((1, 2, every), (3, 0, ())))

    def p_copy(h, i):
        lo, n = COLS[i]
        at = pl.ds(0, 64), pl.ds(lo, n)
        return pltpu.make_async_remote_copy(
            src_ref=part.at[h, *at], dst_ref=rp.at[h, *at],
            send_sem=p_send.at[h, i], recv_sem=p_recv.at[h, i], device_id={"head": partner}, device_id_type=MESH)

    def project(h):
        for g in range(0, G, 2):
            pair = []
            for e in range(2):
                o = acc[:, cols(h, g + e)]
                pair.append((o[0:64] * (1.0 / o[64:65])).astype(bf16))
            mixed[:, g * 64 : (g + 2) * 64] = jnp.concatenate(pair, axis=0).T
        lhs = jnp.concatenate(
            [mixed[pl.ds(pl.multiple_of(32 * i + 16 * c, 16), 16), :] for c in (1 - core, core) for i in range(NX)], axis=0)
        for i, (lo, n) in enumerate(COLS):
            part[h, :, lo : lo + n] = jnp.dot(lhs, wt[:, lo : lo + n], preferred_element_type=f32).astype(bf16)
            p_copy(h, i).start()

    chip = head // 2
    far, up, down = [lax.rem(chip + d, NX) for d in (2, 1, 3)]
    x_up, x_down = xs[0], xs[2]
    lo_c, hi_c = slice(0, SPLIT), slice(SPLIT, D)
    lo_d, hi_d = pl.ds(0, SPLIT), pl.ds(SPLIT, D - SPLIT)

    def x_copy(h, n):
        src, dst, where = (
            (snd.at[h, 0, :, lo_d], rbuf.at[h, :, lo_d], x_up),
            (snd.at[h, 0, :, hi_d], rbuf.at[h, :, hi_d], x_down),
            (snd.at[h, 1, :, hi_d], fin.at[h, 0, :, hi_d], x_up),
            (snd.at[h, 2, :, lo_d], fin.at[h, 1, :, lo_d], x_down),
            (snd.at[h, 1, :, lo_d], fin.at[h, 0, :, lo_d], x_up),
            (snd.at[h, 2, :, hi_d], fin.at[h, 1, :, hi_d], x_down),
        )[n]
        return pltpu.make_async_remote_copy(
            src_ref=src, dst_ref=dst, send_sem=x_send.at[h, n], recv_sem=x_recv.at[h, n],
            device_id={"head": where}, device_id_type=MESH)

    def pair_sums(h):
        for i in range(len(COLS)):
            p_copy(h, i).wait_recv()

        def chip_sum(i):
            at = pl.ds(pl.multiple_of(16 * i, 16), 16)
            own_at = pl.ds(pl.multiple_of(64 + 16 * i, 16), 16)
            return part[h, own_at, :].astype(f32) + rp[h, at, :].astype(f32)

        snd[h, 0] = chip_sum(far).astype(bf16)
        x_copy(h, 0).start()
        x_copy(h, 1).start()
        s_up = chip_sum(up)
        snd[h, 1, :, hi_c] = s_up[:, hi_c].astype(bf16)
        x_copy(h, 2).start()
        s_down = chip_sum(down)
        snd[h, 2, :, lo_c] = s_down[:, lo_c].astype(bf16)
        x_copy(h, 3).start()
        keep[h, 0] = chip_sum(chip)
        keep[h, 1, :, lo_c] = s_up[:, lo_c]
        keep[h, 1, :, hi_c] = s_down[:, hi_c]

    def pass_sums(h):
        for n, row, at in ((0, 1, lo_c), (1, 2, hi_c)):
            x_copy(h, n).wait_recv()
            snd[h, row, :, at] = (keep[h, 1, :, at] + rbuf[h, :, at].astype(f32)).astype(bf16)
            x_copy(h, 4 + n).start()

    def last_sums(h):
        for n in (2, 3, 4, 5):
            x_copy(h, n).wait_recv()
        proj_out[16 * h : 16 * h + 16, :] = (keep[h, 0] + (fin[h, 0].astype(f32) + fin[h, 1].astype(f32))).astype(bf16)

    group(((2, 2, every), (3, 1, every), (3, 3, every), (3, 2, every)), (lambda: project(0), lambda: pl.when(core == 0)(lambda: pair_sums(0))))
    project(1)
    pl.when(core == 1)(lambda: pair_sums(0))
    pl.when(core == 0)(lambda: pair_sums(1))
    band_layer()
    pl.when(core == 1)(lambda: pair_sums(1))
    pass_sums(0)
    pass_sums(1)
    last_sums(0)
    last_sums(1)

    for i in (SEG, K_ROWS, V_ROWS):
        for k in range(3):
            pl.when(z_guard(k))(lambda: z_copy(k, i).wait_send())
        for k in range(4):
            for d in (1, 2, 3):
                pl.when(y_guard(k, d))(lambda: y_copy(k, d, i).wait_send())

    for n in range(3):
        @pl.when(halo_guards[n])
        def _(n=n):
            for i in range(2):
                halo_copy(n, i).wait_send()

    for h in range(2):
        for i in range(len(COLS)):
            p_copy(h, i).wait_send()
        for n in range(6):
            x_copy(h, n).wait_send()


def body(n_ctx, bq, bk, bv, fq, fk, fv, seg, pos, w):
    vmem = pl.BlockSpec(memory_space=pltpu.VMEM)
    dma = pltpu.SemaphoreType.DMA
    band, proj = pl.pallas_call(
        functools.partial(kernel, n_ctx),
        out_shape=(pltpu.VMEM((T, G * HEAD_DIM), bf16), pltpu.VMEM((32, D), bf16)),
        in_specs=[pl.BlockSpec(memory_space=pl.ANY)] * 9,
        out_specs=(vmem, vmem),
        scratch_shapes=[
            pltpu.VMEM((T, 512), bf16),
            pltpu.VMEM((64, T), bf16),
            pltpu.VMEM((64, T), bf16),
            pltpu.VMEM((T, 512), bf16),
            pltpu.VMEM((64, T), bf16),
            pltpu.VMEM((64, T), bf16),
            pltpu.VMEM((1, T), jnp.int32),
            pltpu.VMEM((1, T), jnp.int32),
            pltpu.VMEM((13, 144, T), bf16),
            pltpu.VMEM((13, 1, T), jnp.int32),
            pltpu.VMEM((NY * T, 128), bf16),
            pltpu.VMEM((128, 2048), bf16),
            pltpu.VMEM((128, 2048), bf16),
            pltpu.VMEM((144, T), bf16),
            pltpu.VMEM((128, 128), bf16),
            pltpu.VMEM((1, 128), jnp.int32),
            pltpu.VMEM((128, 128), bf16),
            pltpu.VMEM((1, 128), jnp.int32),
            pltpu.VMEM((384, 128), bf16),
            pltpu.VMEM((T, T), f32),
            pltpu.VMEM((T, T), f32),
            pltpu.VMEM((8, 2048), f32),
            pltpu.VMEM((80, 2048), f32),
            pltpu.VMEM((128, 512), bf16),
            pltpu.VMEM((D, 512), bf16),
            pltpu.VMEM((512, D), bf16),
            pltpu.VMEM((2, 128, D), bf16),
            pltpu.VMEM((2, 64, D), bf16),
            pltpu.VMEM((2, 3, 16, D), bf16),
            pltpu.VMEM((2, 16, D), bf16),
            pltpu.VMEM((2, 2, 16, D), bf16),
            pltpu.VMEM((2, 2, 16, D), f32),
            dma((9,)),
            dma((3, 3)),
            dma((4, 3, 3)),
            dma((12, 3)),
            dma((3, 2)),
            dma((2, 2)),
            dma((2, len(COLS))),
            dma((2, len(COLS))),
            dma((2, 6)),
            dma((2, 6)),
        ],
        compiler_params=pltpu.CompilerParams(
            collective_id=0, has_side_effects=True, vmem_limit_bytes=60000 * 1024),
        name="packed_attention",
    )(bq, bk.T, bv.T, fq, fk.T, fv.T, seg.reshape(1, T), pos.reshape(1, T), w.T)

    def hand_over(band_in, proj_in, band_to, proj_to, sems):
        copies = [
            pltpu.make_async_copy(src, dst, sems.at[i])
            for i, (src, dst) in enumerate(((band_in, band_to), (proj_in, proj_to)))
        ]
        for c in copies:
            c.start()
        for c in copies:
            c.wait()

    hbm = pl.BlockSpec(memory_space=pl.ANY)
    return pl.pallas_call(
        hand_over,
        out_shape=(jax.ShapeDtypeStruct((T, G * HEAD_DIM), bf16), jax.ShapeDtypeStruct((32, D), bf16)),
        in_specs=[hbm, hbm],
        out_specs=(hbm, hbm),
        scratch_shapes=[dma((2,))],
        compiler_params=pltpu.CompilerParams(vmem_limit_bytes=1024 * 1024),
        name="hand_over",
    )(band, proj)


def solution(mesh):
    return jax.shard_map(
        functools.partial(body, mesh.shape["ctx"]),
        mesh=mesh,
        in_specs=(
            P("ctx", "head"),
            P("ctx", "head"),
            P("ctx", "head"),
            P("ctx", "head"),
            P("ctx", "head"),
            P("ctx", "head"),
            P("ctx"),
            P("ctx"),
            P("head", None),
        ),
        out_specs=(P("ctx", "head"), P(("ctx", "head"), None)),
        check_vma=False,
    )
```
